32 devices in a mesh: expert: 16 (over z, y, x), tensor: 2 (over core).
Axes of the slice: x: 2, y: 2, z: 4, core: 2. Of those that a mesh axis runs over, the one named last changes fastest.
Arguments:
- grad_out: bfloat16 [256, 3584], P('expert'), may hold values from -1.5 to 1.5
- expert_ids: int32 [256, 8], P('expert'), may hold values from 0 to 15, all different within a row; in each aligned block of 16 rows (0 to 15, 16 to 31, ...) at most 16 rows name the same one
- gate_values: float32 [256, 8], P('expert'), may hold values from 0.05 to 0.6
- w_gate_up: bfloat16 [16, 2, 3584, 1024], P('expert', None, None, 'tensor'), may hold values from -0.09375 to 0.09375
- w_down: bfloat16 [16, 1024, 3584], P('expert', 'tensor'), may hold values from -0.1875 to 0.1875
- saved_routed: bfloat16 [16, 2, 256, 1024], P('expert', None, None, 'tensor'), may hold values from -6 to 6
- shared_gate_up: bfloat16 [2, 3584, 1024], P(None, 'expert', 'tensor'), may hold values from -0.09375 to 0.09375
- shared_down: bfloat16 [1024, 3584], P('tensor', 'expert'), may hold values from -0.1875 to 0.1875
- saved_shared: bfloat16 [2, 256, 1024], P(None, 'expert', 'tensor'), may hold values from -6 to 6
Outputs:
- grad_in: bfloat16 [256, 3584], P('expert', 'tensor')
- grad_gates: float32 [256, 8], P('expert')
The draws below stay inside these ranges and needn't reach their ends.
Inputs may be any that keep to these rules, and one draw needn't show every extreme that they name: `expert_ids`: each row names 8 different experts. Among the 16 rows of one index of expert (aligned blocks of rows), no expert is named by more than 16 rows, and in some block one expert is named by exactly 16 rows.
All inputs are finite; a program needn't handle non-finite values.
Results may differ from the reference program's by a relative error of at most 0.015.
Values may be sent and summed in bfloat16 or wider, within the bound.
A program may use at most 64 MiB of HBM per device.

```python
import math
import jax
import jax.numpy as jnp
import numpy as np
from jax import lax

D = 3584
FF = 1024
FF_SH = 1024
TOP = 8
TOK_DEV = 16
EXPERTS = 16
CAP = 16
SLOTS = 256
TOKENS = 256
N_EXPERT = 16
N_TENSOR = 2


def block_scale(own_key, extent, shards, smallest, largest):
    factor_of = 1.0
    for dim, parts in shards:
        heights = jax.random.uniform(jax.random.fold_in(jax.random.fold_in(own_key, 6), dim), (parts,), jnp.float32, smallest / len(shards), largest / len(shards))
        factor_of = factor_of * jnp.repeat(jnp.exp(heights), extent[dim] // parts).reshape((-1,) + (1,) * (len(extent) - 1 - dim))
    return factor_of


def deal_out(rng, own, number, rows, count, top, bound, slope):
    ranking = jax.random.permutation(rng, count)
    crowded, usual = shares(count, rows * top, bound, slope, True), shares(count, rows * top, bound, slope, False)
    places = jnp.arange(count)

    def named(lengths, rotation):
        used = int((lengths > 0).sum())
        fixed = max(1, used // 4)
        passed = fixed + (places - fixed + rotation * (used - fixed)) % max(1, count - fixed)
        return jnp.zeros((count,), jnp.int32).at[ranking[jnp.where(places < fixed, places, passed)]].set(jnp.asarray(lengths, jnp.int32))

    lengths = jnp.where(number % 4 == 0, named(crowded, number // 4), named(usual, number - number // 4 - 1))
    mixed = jax.random.permutation(jax.random.fold_in(own, 3), count)
    donor, taker = mixed[0:count // 2 * 2:2], mixed[1:count // 2 * 2:2]
    room = jnp.minimum(lengths[donor] - 1, bound - lengths[taker]) // 2
    room = jnp.where((donor == ranking[0]) | (taker == ranking[0]) | (lengths[taker] == 0), 0, jnp.maximum(room, 0))
    passed = jax.random.randint(jax.random.fold_in(own, 4), (count // 2,), 0, 1 << 20) % (room + 1)
    lengths = lengths.at[donor].add(-passed).at[taker].add(passed)
    items = jnp.searchsorted(jnp.cumsum(lengths), jnp.arange(rows * top), side="right").astype(jnp.int32)
    table = items.reshape(top, rows).T
    table = table[jax.random.permutation(jax.random.fold_in(own, 1), rows)]
    rotation = jax.random.randint(jax.random.fold_in(own, 2), (rows, 1), 0, top)
    return jnp.take_along_axis(table, (jnp.arange(top)[None, :] + rotation) % top, axis=1)


def shares(count, total, reach, lean, full):
    weights = [(1 << 20) // math.isqrt(grade ** lean) + 1 for grade in range(1, count + 1)]
    largest = reach if full else min(reach, max(-(-total // count), total * weights[0] // sum(weights)))
    least = 1 if total - largest >= count - 1 else 0
    counts, rest = [largest] + [least] * (count - 1), total - largest - least * (count - 1)
    while rest > 0:
        candidates = [i for i in range(1, count) if counts[i] < largest] or [i for i in range(1, count) if counts[i] < reach]
        mass, left = sum([weights[i] for i in candidates]), rest
        for i in candidates:
            extra = min(reach - counts[i], max(1, left * weights[i] // mass), rest)
            counts[i] = counts[i] + extra
            rest = rest - extra
    return np.array(counts)


def scatter_about(rng, shape, width, limit, pieces=(), kind=jnp.bfloat16):
    entries = jax.random.normal(rng, shape, jnp.float32) * width
    if len(pieces) > 0:
        entries = block_scale(rng, shape, pieces, -0.22, 0.18) * entries
    return jnp.clip(entries, min=-limit, max=limit).astype(kind)


def setup_inputs(seed: int = 0) -> dict:
    key_of = jax.random.split(jax.random.key(seed), 10)
    grad_out = scatter_about(key_of[0], (TOKENS, D), 0.25, 1.5, ((0, 16),))
    expert_ids_keys = jax.random.split(jax.random.fold_in(key_of[1], 1), TOKENS // TOK_DEV)
    expert_ids_turns = jax.random.permutation(jax.random.fold_in(key_of[1], 3), TOKENS // TOK_DEV)
    expert_ids = jax.vmap(lambda own, number: deal_out(jax.random.fold_in(key_of[1], 2), own, number, TOK_DEV, EXPERTS, TOP, CAP, 2))(expert_ids_keys, expert_ids_turns).reshape((TOKENS, TOP))
    gate_values = jnp.clip(jnp.exp(math.log(0.6) - 2.4849067 * jax.random.uniform(key_of[2], (TOKENS, TOP), jnp.float32) ** block_scale(key_of[2], (TOKENS, TOP), ((0, 16),), -0.2, 0.2)), 0.05, 0.6)
    w_gate_up = scatter_about(key_of[3], (EXPERTS, 2, D, FF), D ** -0.5, 0.09375, ((0, 16), (3, 2)))
    w_down = scatter_about(key_of[4], (EXPERTS, FF, D), FF ** -0.5, 0.1875, ((0, 16), (1, 2)))
    saved_routed = scatter_about(key_of[5], (EXPERTS, 2, SLOTS, FF), 1.0, 6.0, ((0, 16), (3, 2)))
    shared_gate_up = scatter_about(key_of[6], (2, D, FF_SH), D ** -0.5, 0.09375, ((1, 16), (2, 2)))
    shared_down = scatter_about(key_of[7], (FF_SH, D), FF_SH ** -0.5, 0.1875, ((0, 2), (1, 16)))
    saved_shared = scatter_about(key_of[8], (2, TOKENS, FF_SH), 1.0, 6.0, ((1, 16), (2, 2)))
    return {"grad_out": grad_out, "expert_ids": expert_ids, "gate_values": gate_values, "w_gate_up": w_gate_up, "w_down": w_down, "saved_routed": saved_routed, "shared_gate_up": shared_gate_up, "shared_down": shared_down, "saved_shared": saved_shared}


def swiglu_grads(back_grad, saved_gate, saved_up):
    pre_gate = saved_gate.astype(jnp.float32)
    pre_up = saved_up.astype(jnp.float32)
    sigmoid = jax.nn.sigmoid(pre_gate)
    grad_gate = (back_grad * pre_up * sigmoid * (1.0 + pre_gate * (1.0 - sigmoid))).astype(jnp.bfloat16)
    grad_up = (back_grad * pre_gate * sigmoid).astype(jnp.bfloat16)
    return grad_gate, grad_up


def gate_mixture(back_grad, saved_gate, saved_up):
    pre_gate = saved_gate.astype(jnp.float32)
    pre_up = saved_up.astype(jnp.float32)
    sigmoid = jax.nn.sigmoid(pre_gate)
    return back_grad * pre_gate * sigmoid * pre_up


def slot_numbers(expert_ids):
    blocks = expert_ids.reshape(N_EXPERT, TOK_DEV * TOP).astype(jnp.int32)
    onehot = (blocks[:, :, None] == jnp.arange(EXPERTS, dtype=jnp.int32)[None, None, :]).astype(jnp.int32)
    earlier = (jnp.cumsum(onehot, axis=1) - onehot).astype(jnp.int32)
    position = jnp.sum(earlier * onehot, axis=2).astype(jnp.int32)
    offsets = jnp.arange(N_EXPERT, dtype=jnp.int32)[:, None] * CAP
    return (offsets + position).reshape(-1).astype(jnp.int32)


def reference(grad_out, expert_ids, gate_values, w_gate_up, w_down, saved_routed, shared_gate_up, shared_down, saved_shared):
    slot_flat = slot_numbers(expert_ids)
    ids_flat = expert_ids.reshape(-1).astype(jnp.int32)
    pair_token = (jnp.arange(TOKENS * TOP, dtype=jnp.int32) // TOP).astype(jnp.int32)
    source_table = jnp.full((EXPERTS, SLOTS), TOKENS, jnp.int32).at[ids_flat, slot_flat].set(pair_token)
    gate_table = jnp.zeros((EXPERTS, SLOTS), jnp.float32).at[ids_flat, slot_flat].set(gate_values.reshape(-1).astype(jnp.float32))
    padded = jnp.concatenate([grad_out, jnp.zeros((1, D), grad_out.dtype)], axis=0)
    slice_width = FF // N_TENSOR

    def one_expert(running, inputs):
        weights_gu, weights_down, saved_pre, source_row, gate_row = inputs
        slot_rows = padded[source_row]
        back_grad = jnp.dot(slot_rows, weights_down.T, preferred_element_type=jnp.float32)
        grad_gate, grad_up = swiglu_grads(back_grad, saved_pre[0], saved_pre[1])
        gate_mix = gate_mixture(back_grad, saved_pre[0], saved_pre[1])
        row_sum = jnp.zeros((SLOTS, D), jnp.float32)
        gate_sum = jnp.zeros((SLOTS,), jnp.float32)
        for slice_index in range(N_TENSOR):
            lower_edge = slice_index * slice_width
            upper_edge = lower_edge + slice_width
            slice_term = jnp.dot(grad_gate[:, lower_edge:upper_edge], weights_gu[0][:, lower_edge:upper_edge].T, preferred_element_type=jnp.float32)
            slice_term = slice_term + jnp.dot(grad_up[:, lower_edge:upper_edge], weights_gu[1][:, lower_edge:upper_edge].T, preferred_element_type=jnp.float32)
            slice_term = lax.optimization_barrier(slice_term.astype(jnp.bfloat16))
            row_sum = row_sum + slice_term.astype(jnp.float32)
            gate_piece = lax.optimization_barrier(jnp.sum(gate_mix[:, lower_edge:upper_edge], axis=1).astype(jnp.bfloat16))
            gate_sum = gate_sum + gate_piece.astype(jnp.float32)
        running = running.at[source_row].add(gate_row[:, None] * row_sum)
        return running, gate_sum

    initial = jnp.zeros((TOKENS + 1, D), jnp.float32)
    routed, gate_sums = lax.scan(one_expert, initial, (w_gate_up, w_down, saved_routed, source_table, gate_table))
    grad_gates = gate_sums[ids_flat, slot_flat].reshape(TOKENS, TOP)
    shared_back = jnp.dot(grad_out, shared_down.T, preferred_element_type=jnp.float32)
    shared_gate, shared_up = swiglu_grads(shared_back, saved_shared[0], saved_shared[1])
    shared_term = jnp.dot(shared_gate, shared_gate_up[0].T, preferred_element_type=jnp.float32)
    shared_term = shared_term + jnp.dot(shared_up, shared_gate_up[1].T, preferred_element_type=jnp.float32)
    grad_in = (routed[:TOKENS] + shared_term).astype(jnp.bfloat16)
    return grad_in, grad_gates
```

```python
import functools

import jax
import jax.numpy as jnp
from jax import lax
from jax.experimental import pallas as pl
from jax.experimental.pallas import tpu as pltpu
from jax.sharding import PartitionSpec as P

MESH = pl.DeviceIdType.MESH
LANES = 128


def dot_nt(left, right):
    return lax.dot_general(
        left, right, (((1,), (1,)), ((), ())), preferred_element_type=jnp.float32
    )


def loop(count, body):
    def step(i, carry):
        body(i)
        return carry

    lax.fori_loop(0, count, step, 0)


def flat(value):
    return value.reshape(-1, value.shape[-1])


def kernel(
    E, T, F, NC, TOP,
    g_ref, x_ref, m_ref, sv_ref, sgu_ref, sd_ref, wd_hbm, wgu_hbm, sr_hbm,
    out_r, out_s, out_g,
    gbuf, xbuf, mbuf, wd, wgu, sr,
    ps, s2buf, s3buf, st, s4buf, s4pair, gm, gmbuf, gpair,
    pairsend, pairbuf, part, r3buf, r2buf, rzbuf,
    wsem, g_recv, g_sz, g_s2, g_s3, g_ps, g_pr,
    s3_recv, s3_sz, s3_s2, s3_s3,
    x_s, x_r, m_s, m_r, s2_s, s2_r, s4_s, s4_r, gm_s, gm_r,
    s4p_s, s4p_r, gp_s, gp_r, pair_s, pair_r,
    r3_s, r3_r, r2_s, r2_r, rz_s, rz_r,
):
    me = lax.axis_index("expert")
    j = lax.axis_index("tensor")
    A = E // 4
    a = me // 4
    r = me % 4
    rc = r + 1 - 2 * (r % 2)
    rb = r + 2 - 4 * (r // 2)
    odd = j % 2
    r2 = rc * (1 - odd) + rb * odd
    r3 = rb * (1 - odd) + rc * odd
    r23 = 3 - r
    p2 = a * 4 + r2
    p3 = a * 4 + r3
    fj = j if F > 1 else 0
    tok = x_ref.shape[1]
    FFl = wd.shape[0]
    H = g_ref.shape[2]
    HR = part.shape[3] * NC
    HC = part.shape[3]
    tokens = E * tok

    def rc_(src, dst, ssem, rsem, chip, core):
        return pltpu.make_async_remote_copy(
            src_ref=src, dst_ref=dst, send_sem=ssem, recv_sem=rsem,
            device_id=(chip, core), device_id_type=MESH,
        )

    wcopies = [
        pltpu.make_async_copy(sr_hbm, sr, wsem.at[0]),
        pltpu.make_async_copy(wd_hbm, wd, wsem.at[1]),
        pltpu.make_async_copy(wgu_hbm, wgu, wsem.at[2]),
    ]
    for copy in wcopies:
        copy.start()

    barrier = pltpu.get_barrier_semaphore()

    def greet(i):
        pl.semaphore_signal(barrier, inc=1, device_id=((me + i + 1) % E, j), device_id_type=MESH)

    loop(E - 1, greet)
    for d in range(1, T):
        pl.semaphore_signal(barrier, inc=1, device_id=(me, (j + d) % T), device_id_type=MESH)
    pl.semaphore_wait(barrier, E - 1 + T - 1)

    def a2a_send(src_of, dst, ssem, rsem):
        def body(i):
            o = (me + i + 1) % E
            rc_(src_of(o), dst.at[me], ssem.at[o], rsem.at[me], o, j).start()

        loop(E - 1, body)

    def a2a_wait(dst, rsem):
        def body(i):
            o = (me + i + 1) % E
            rc_(dst.at[o], dst.at[o], rsem.at[o], rsem.at[o], o, j).wait_recv()

        loop(E - 1, body)

    def a2a_drain(src_of, ssem):
        def body(i):
            o = (me + i + 1) % E
            rc_(src_of(o), src_of(o), ssem.at[o], ssem.at[o], o, j).wait_send()

        loop(E - 1, body)

    class Tree:
        def __init__(self, buf, own, recv, sz, s2, s3, hook):
            self.buf, self.own, self.recv = buf, own, recv
            self.sz, self.s2, self.s3, self.hook = sz, s2, s3, hook

        def send(self, blk, ssem, chip, src=None):
            src = self.buf.at[blk] if src is None else src
            rc_(src, self.buf.at[blk], ssem, self.recv.at[blk], chip, j).start()

        def wait(self, blk):
            rc_(self.buf.at[blk], self.buf.at[blk], self.recv.at[blk], self.recv.at[blk], p2, j).wait_recv()

        def start(self):
            self.send(me, self.s3.at[0], p3, self.own)
            self.send(me, self.s2.at[0], p2, self.own)

            def body(i):
                self.send(me, self.sz.at[i], ((a + i + 1) % A) * 4 + r, self.own)

            loop(A - 1, body)
            self.hook(me, self.own)

        def stage_z(self):
            def body(i):
                blk = ((a + i + 1) % A) * 4 + r
                self.wait(blk)
                self.send(blk, self.s3.at[i + 1], p3)
                self.send(blk, self.s2.at[i + 1], p2)
                self.hook(blk, self.buf.at[blk])

            loop(A - 1, body)

        def stage_2(self):
            def body(i):
                blk = ((a + i) % A) * 4 + r2
                self.wait(blk)
                self.send(blk, self.s3.at[A + i], p3)
                self.hook(blk, self.buf.at[blk])

            loop(A, body)

        def stage_3(self):
            for rr in (r3, r23):
                def body(i):
                    blk = ((a + i) % A) * 4 + rr
                    self.wait(blk)
                    self.hook(blk, self.buf.at[blk])

                loop(A, body)

        def drain(self):
            def one(sem):
                rc_(self.own, self.own, sem, sem, p2, j).wait_send()

            loop(A - 1, lambda i: one(self.sz.at[i]))
            loop(A, lambda i: one(self.s2.at[i]))
            loop(2 * A, lambda i: one(self.s3.at[i]))

    def pair_hook(blk, src):
        if F > 1:
            for d in range(1, T):
                rc_(
                    src, gbuf.at[j, blk], g_ps.at[d, blk], g_pr.at[j, blk], me, (j + d) % T
                ).start()

    tree_g = Tree(gbuf.at[fj], g_ref.at[fj], g_recv, g_sz, g_s2, g_s3, pair_hook)
    tree_s = Tree(s3buf, s3buf.at[me], s3_recv, s3_sz, s3_s2, s3_s3, lambda blk, src: None)

    a2a_send(lambda o: x_ref.at[o], xbuf, x_s, x_r)
    tree_g.start()
    a2a_send(lambda o: m_ref, mbuf, m_s, m_r)
    xbuf[me] = x_ref[me]
    mbuf[me] = m_ref[...]
    gbuf[fj, me] = g_ref[fj]

    a2a_wait(xbuf, x_r)
    ps[...] = dot_nt(flat(xbuf[...]), sd_ref[...]).astype(jnp.bfloat16).reshape(E, tok, FFl)
    a2a_send(lambda o: ps.at[o], s2buf, s2_s, s2_r)
    s2buf[me] = ps[me]

    tree_g.stage_z()

    a2a_wait(mbuf, m_r)
    meta = flat(mbuf[...])
    lane = lax.broadcasted_iota(jnp.int32, (tokens, LANES), 1)
    hit = jnp.where((meta == me.astype(jnp.float32)) & (lane < TOP), 1.0, 0.0)
    gates = pltpu.roll(meta, LANES - TOP, 1)
    chosen = jnp.sum(hit, axis=1, keepdims=True)
    gate = jnp.sum(hit * gates, axis=1, keepdims=True)
    wide = jnp.broadcast_to(chosen, (tokens, LANES))
    row = lax.broadcasted_iota(jnp.int32, (tokens, LANES), 0) % tok
    total = wide
    shift = 1
    while shift < tok:
        total = total + jnp.where(row >= shift, pltpu.roll(total, shift, 0), 0.0)
        shift *= 2
    position = (total - wide)[:, :1]
    slots = sr.shape[1]
    cap = slots // E
    base = (lax.broadcasted_iota(jnp.int32, (tokens, 1), 0) // tok) * cap
    target = position + base.astype(jnp.float32)
    slot = lax.broadcasted_iota(jnp.int32, (tokens, slots), 1).astype(jnp.float32)
    permute = jnp.where((slot == target) & (chosen > 0.5), 1.0, 0.0).astype(jnp.bfloat16)

    tree_g.stage_2()

    wcopies[0].wait()
    pre_gate = jnp.dot(permute, sr[0], preferred_element_type=jnp.float32)
    pre_up = jnp.dot(permute, sr[1], preferred_element_type=jnp.float32)
    sig = jax.nn.sigmoid(pre_gate)
    d_up = pre_gate * sig
    d_gate = pre_up * sig * (1.0 + pre_gate * (1.0 - sig))

    a2a_wait(s2buf, s2_r)
    shared_back = jnp.sum(s2buf[...].astype(jnp.float32), axis=0)
    sh = sv_ref[0].astype(jnp.float32)
    su = sv_ref[1].astype(jnp.float32)
    ssig = jax.nn.sigmoid(sh)
    s3buf[me, 0] = (shared_back * su * ssig * (1.0 + sh * (1.0 - ssig))).astype(jnp.bfloat16)
    s3buf[me, 1] = (shared_back * sh * ssig).astype(jnp.bfloat16)
    tree_s.start()

    tree_g.stage_3()
    tree_s.stage_z()

    wcopies[1].wait()
    if F > 1:
        back = jnp.zeros((tokens, FFl), jnp.float32)
        for d in range(1, T):
            other = (j + d) % T

            def body(i):
                ref = gbuf.at[other, i]
                rc_(ref, ref, g_pr.at[other, i], g_pr.at[other, i], me, other).wait_recv()

            loop(E, body)
        for t in range(F):
            back = back + dot_nt(flat(gbuf[t]), wd[:, t * H:(t + 1) * H])
    else:
        back = dot_nt(flat(gbuf[0]), wd[...])
    tree_s.stage_2()
    grad_up = back * d_up
    gate_sum = jnp.sum(grad_up * pre_up, axis=1, keepdims=True)
    gate_sum = gate_sum.astype(jnp.bfloat16).astype(jnp.float32)
    grad_gate = (back * d_gate * gate).astype(jnp.bfloat16)
    grad_up = (grad_up * gate).astype(jnp.bfloat16)
    gm[...] = jnp.where(lane == me, gate_sum, 0.0).reshape(E, tok, LANES)
    a2a_send(lambda o: gm.at[o], gmbuf, gm_s, gm_r)
    gmbuf[me] = gm[me]

    wcopies[2].wait()

    def rows_of(t, c):
        span = pl.ds(pl.multiple_of(t * HR + c * HC, 16), HC)
        return dot_nt(grad_gate, wgu[0, span, :]) + dot_nt(grad_up, wgu[1, span, :])

    for c in range(NC):
        for d in range(1, T):
            t = (j + d) % T
            pairsend[d - 1, c] = rows_of(t, c).astype(jnp.bfloat16)
            rc_(
                pairsend.at[d - 1, c], pairbuf.at[T - 1 - d, c],
                pair_s.at[d - 1, c], pair_r.at[T - 1 - d, c], me, t,
            ).start()

    def stage3_blocks(c, i):
        ap = i // 2
        w = i % 2
        blk = ap * 4 + r3 * (1 - w) + r23 * w
        return rc_(part.at[c, blk], r3buf.at[c, i], r3_s.at[c, i], r3_r.at[c, i], p3, j)

    for c in range(NC):
        mine = rows_of(j, c)
        for d in range(1, T):
            rc_(
                pairsend.at[d - 1, c], pairbuf.at[d - 1, c],
                pair_s.at[d - 1, c], pair_r.at[d - 1, c], me, (j + d) % T,
            ).wait_recv()
            mine = mine + pairbuf[d - 1, c].astype(jnp.float32)
        part[c] = mine.astype(jnp.bfloat16).reshape(E, tok, HC)
        loop(2 * A, lambda i: stage3_blocks(c, i).start())

    tree_s.stage_3()
    term = dot_nt(flat(s3buf[:, 0]), sgu_ref[0]) + dot_nt(flat(s3buf[:, 1]), sgu_ref[1])
    st[...] = term.astype(jnp.bfloat16).reshape(E, tok, st.shape[2])
    a2a_send(lambda o: st.at[o], s4buf, s4_s, s4_r)
    s4buf[me] = st[me]

    def stage2_block(c, i):
        return rc_(part.at[c, i * 4 + r2], r2buf.at[c, i], r2_s.at[c, i], r2_r.at[c, i], p2, j)

    for c in range(NC):
        loop(2 * A, lambda i: stage3_blocks(c, i).wait_recv())

        def add_first(i):
            blk = i * 4 + r2
            part[c, blk] = (
                part[c, blk].astype(jnp.float32) + r3buf[c, i * 2 + 1].astype(jnp.float32)
            ).astype(jnp.bfloat16)

        loop(A, add_first)
        loop(A, lambda i: stage2_block(c, i).start())

    def stagez_block(c, i):
        o = (a + i + 1) % A
        return rc_(
            part.at[c, o * 4 + r], rzbuf.at[c, a], rz_s.at[c, o], rz_r.at[c, a], o * 4 + r, j
        )

    for c in range(NC):
        loop(A, lambda i: stage2_block(c, i).wait_recv())

        def add_second(i):
            blk = i * 4 + r
            part[c, blk] = (
                part[c, blk].astype(jnp.float32)
                + r3buf[c, i * 2].astype(jnp.float32)
                + r2buf[c, i].astype(jnp.float32)
            ).astype(jnp.bfloat16)

        loop(A, add_second)
        loop(A - 1, lambda i: stagez_block(c, i).start())
        rzbuf[c, a] = part[c, me]

    a2a_wait(gmbuf, gm_r)
    gpair[T - 1] = jnp.sum(gmbuf[...], axis=0)
    a2a_wait(s4buf, s4_r)
    group = E // T
    for d in range(1, T):
        t = (j + d) % T
        rc_(gpair.at[T - 1], gpair.at[T - 1 - d], gp_s.at[d - 1], gp_r.at[T - 1 - d], me, t).start()
        rc_(
            s4buf.at[pl.ds(t * group, group)], s4pair.at[T - 1 - d],
            s4p_s.at[d - 1], s4p_r.at[T - 1 - d], me, t,
        ).start()
    shared = s4buf[pl.ds(j * group, group)].astype(jnp.float32)
    for d in range(1, T):
        rc_(gpair.at[T - 1], gpair.at[d - 1], gp_s.at[d - 1], gp_r.at[d - 1], me, (j + d) % T).wait_recv()
        rc_(
            s4pair.at[d - 1], s4pair.at[d - 1], s4p_s.at[d - 1], s4p_r.at[d - 1], me, (j + d) % T
        ).wait_recv()
        shared = shared + s4pair[d - 1].astype(jnp.float32)
    out_s[...] = shared
    sums = jnp.sum(gpair[...], axis=0)
    own_meta = m_ref[...]
    lane16 = lax.broadcasted_iota(jnp.int32, (tok, LANES), 1)
    lane_f = lane16.astype(jnp.float32)
    result = jnp.zeros((tok, LANES), jnp.float32)
    for k in range(TOP):
        value = jnp.sum(
            jnp.where(lane_f == own_meta[:, k:k + 1], sums, 0.0), axis=1, keepdims=True
        )
        result = jnp.where(lane16 == k, value, result)
    out_g[...] = result

    for c in range(NC):
        def wait_z(i):
            o = (a + i + 1) % A
            rc_(rzbuf.at[c, o], rzbuf.at[c, o], rz_s.at[c, o], rz_r.at[c, o], p2, j).wait_recv()

        loop(A - 1, wait_z)
        out_r[c] = jnp.sum(rzbuf[c].astype(jnp.float32), axis=0)

    a2a_drain(lambda o: x_ref.at[o], x_s)
    a2a_drain(lambda o: m_ref, m_s)
    a2a_drain(lambda o: ps.at[o], s2_s)
    a2a_drain(lambda o: gm.at[o], gm_s)
    a2a_drain(lambda o: st.at[o], s4_s)
    tree_g.drain()
    tree_s.drain()
    for d in range(1, T):
        if F > 1:
            loop(
                E,
                lambda i: rc_(
                    gbuf.at[j, i], gbuf.at[j, i], g_ps.at[d, i], g_ps.at[d, i], me, (j + d) % T
                ).wait_send(),
            )
        rc_(gpair.at[T - 1], gpair.at[T - 1], gp_s.at[d - 1], gp_s.at[d - 1], me, (j + d) % T).wait_send()
        rc_(
            s4pair.at[d - 1], s4pair.at[d - 1], s4p_s.at[d - 1], s4p_s.at[d - 1], me, (j + d) % T
        ).wait_send()
        for c in range(NC):
            ref = pairsend.at[d - 1, c]
            rc_(ref, ref, pair_s.at[d - 1, c], pair_s.at[d - 1, c], me, (j + d) % T).wait_send()
    for c in range(NC):
        loop(2 * A, lambda i: stage3_blocks(c, i).wait_send())
        loop(A, lambda i: stage2_block(c, i).wait_send())
        loop(A - 1, lambda i: stagez_block(c, i).wait_send())


def per_device(
    E, T,
    grad_out, expert_ids, gate_values, w_gate_up, w_down, saved_routed,
    shared_gate_up, shared_down, saved_shared,
):
    tok, D = grad_out.shape
    TOP = expert_ids.shape[1]
    FFl = w_down.shape[1]
    DS = shared_down.shape[1]
    slots = saved_routed.shape[2]
    F = T if (D // T) % LANES == 0 else 1
    H = D // F
    HR = D // T
    NC = 2 if HR % (2 * LANES) == 0 else 1
    HC = HR // NC
    A = E // 4
    tokens = E * tok
    halves = grad_out.reshape(tok, F, H).transpose(1, 0, 2)
    pieces = grad_out.reshape(tok, E, DS).transpose(1, 0, 2)
    meta = jnp.concatenate(
        [
            expert_ids.astype(jnp.float32),
            gate_values,
            jnp.zeros((tok, LANES - 2 * TOP), jnp.float32),
        ],
        axis=1,
    )
    bf, f32 = jnp.bfloat16, jnp.float32
    V, S = pltpu.VMEM, pltpu.SemaphoreType.DMA
    T1 = max(T - 1, 1)
    scratch = [
        V((F, E, tok, H), bf), V((E, tok, DS), bf), V((E, tok, LANES), f32),
        V((FFl, D), bf), V((2, D, FFl), bf), V((2, slots, FFl), bf),
        V((E, tok, FFl), bf), V((E, tok, FFl), bf), V((E, 2, tok, FFl), bf),
        V((E, tok, DS), bf), V((E, tok, DS), bf), V((T1, E // T, tok, DS), bf),
        V((E, tok, LANES), f32), V((E, tok, LANES), f32), V((T, tok, LANES), f32),
        V((T1, NC, tokens, HC), bf), V((T1, NC, tokens, HC), bf), V((NC, E, tok, HC), bf),
        V((NC, 2 * A, tok, HC), bf), V((NC, A, tok, HC), bf), V((NC, A, tok, HC), bf),
        S((3,)), S((E,)), S((A,)), S((A,)), S((2 * A,)), S((T, E)), S((T, E)),
        S((E,)), S((A,)), S((A,)), S((2 * A,)),
        S((E,)), S((E,)), S((E,)), S((E,)), S((E,)), S((E,)), S((E,)), S((E,)), S((E,)), S((E,)),
        S((T1,)), S((T1,)), S((T1,)), S((T1,)), S((T1, NC)), S((T1, NC)),
        S((NC, 2 * A)), S((NC, 2 * A)), S((NC, A)), S((NC, A)), S((NC, A)), S((NC, A)),
    ]
    vm = pl.BlockSpec(memory_space=pltpu.VMEM)
    hbm = pl.BlockSpec(memory_space=pltpu.HBM)
    routed, shared, gates = pl.pallas_call(
        functools.partial(kernel, E, T, F, NC, TOP),
        out_shape=(
            jax.ShapeDtypeStruct((NC, tok, HC), f32),
            jax.ShapeDtypeStruct((E // T, tok, DS), f32),
            jax.ShapeDtypeStruct((tok, LANES), f32),
        ),
        in_specs=[vm] * 6 + [hbm] * 3,
        out_specs=(vm, vm, vm),
        scratch_shapes=scratch,
        compiler_params=pltpu.CompilerParams(
            collective_id=0, has_side_effects=True, vmem_limit_bytes=60 * 1024 * 1024
        ),
    )(
        halves, pieces, meta, saved_shared, shared_gate_up, shared_down,
        w_down[0], w_gate_up[0], saved_routed[0],
    )
    routed = routed.transpose(1, 0, 2).reshape(tok, HR)
    shared = shared.transpose(1, 0, 2).reshape(tok, HR)
    return (routed + shared).astype(bf), gates[:, :TOP]


def solution(mesh):
    return jax.shard_map(
        functools.partial(per_device, mesh.shape["expert"], mesh.shape["tensor"]),
        mesh=mesh,
        in_specs=(
            P("expert", None),
            P("expert", None),
            P("expert", None),
            P("expert", None, None, "tensor"),
            P("expert", "tensor", None),
            P("expert", None, None, "tensor"),
            P(None, "expert", "tensor"),
            P("tensor", "expert"),
            P(None, "expert", "tensor"),
        ),
        out_specs=(P("expert", "tensor"), P("expert", None)),
        check_vma=False,
    )
```

```python
import functools

import jax
import jax.numpy as jnp
from jax import lax
from jax.experimental import pallas as pl
from jax.experimental.pallas import tpu as pltpu
from jax.sharding import PartitionSpec as P

MESH = pl.DeviceIdType.MESH
LANES = 128


def dot_nt(left, right):
    return lax.dot_general(
        left, right, (((1,), (1,)), ((), ())), preferred_element_type=jnp.float32
    )


def loop(count, body):
    def step(i, carry):
        body(i)
        return carry

    lax.fori_loop(0, count, step, 0)


def flat(value):
    return value.reshape(-1, value.shape[-1])


def kernel(
    E, T, F, NC, TOP,
    g_ref, id_ref, gv_ref, sv_ref, sgu_ref, sd_ref, wd_hbm, wgu_hbm, sr_hbm,
    out_r, out_g,
    x_ref, m_ref, square, spread, gbuf, xbuf, mbuf, wd, wgu, sr,
    ps, s2buf, s3buf, st, s4buf, s4pair, gm, gmbuf, gpair,
    pairsend, pairbuf, part, r3buf, r2buf, rzbuf,
    wsem, g_recv, g_sz, g_s2, g_s3, g_ps, g_pr,
    s3_recv, s3_sz, s3_s2, s3_s3,
    x_s, x_r, m_s, m_r, s2_s, s2_r, s4_s, s4_r, gm_s, gm_r,
    s4p_s, s4p_r, gp_s, gp_r, pair_s, pair_r,
    r3_s, r3_r, r2_s, r2_r, rz_s, rz_r,
):
    me = lax.axis_index("expert")
    j = lax.axis_index("tensor")
    A = E // 4
    a = me // 4
    r = me % 4
    rc = r + 1 - 2 * (r % 2)
    rb = r + 2 - 4 * (r // 2)
    odd = j % 2
    r2 = rc * (1 - odd) + rb * odd
    r3 = rb * (1 - odd) + rc * odd
    r23 = 3 - r
    p2 = a * 4 + r2
    p3 = a * 4 + r3
    fj = j if F > 1 else 0
    tok = x_ref.shape[1]
    DS = x_ref.shape[2]
    FFl = wd.shape[0]
    H = gbuf.shape[3]
    own_g = g_ref.at[:, pl.ds(pl.multiple_of(fj * H, LANES), H)] if F > 1 else g_ref
    HR = part.shape[3] * NC
    HC = part.shape[3]
    tokens = E * tok

    def rc_(src, dst, ssem, rsem, chip, core):
        return pltpu.make_async_remote_copy(
            src_ref=src, dst_ref=dst, send_sem=ssem, recv_sem=rsem,
            device_id=(chip, core), device_id_type=MESH,
        )

    wcopies = [
        pltpu.make_async_copy(sr_hbm, sr, wsem.at[0]),
        pltpu.make_async_copy(wd_hbm, wd, wsem.at[1]),
        pltpu.make_async_copy(wgu_hbm, wgu, wsem.at[2]),
    ]
    for copy in wcopies:
        copy.start()

    barrier = pltpu.get_barrier_semaphore()

    def greet(i):
        pl.semaphore_signal(barrier, inc=1, device_id=((me + i + 1) % E, j), device_id_type=MESH)

    loop(E - 1, greet)
    for d in range(1, T):
        pl.semaphore_signal(barrier, inc=1, device_id=(me, (j + d) % T), device_id_type=MESH)

    for o in range(E):
        x_ref[o] = g_ref[:, o * DS:(o + 1) * DS]
    square[...] = jnp.zeros_like(square)
    square[0:TOP, 0:tok] = id_ref[...].astype(jnp.float32)
    square[TOP:2 * TOP, 0:tok] = gv_ref[...]
    m_ref[...] = square[...].T[0:tok]

    pl.semaphore_wait(barrier, E - 1 + T - 1)

    def a2a_send(src_of, dst, ssem, rsem):
        def body(i):
            o = (me + i + 1) % E
            rc_(src_of(o), dst.at[me], ssem.at[o], rsem.at[me], o, j).start()

        loop(E - 1, body)

    def a2a_wait(dst, rsem):
        def body(i):
            o = (me + i + 1) % E
            rc_(dst.at[o], dst.at[o], rsem.at[o], rsem.at[o], o, j).wait_recv()

        loop(E - 1, body)

    def a2a_drain(src_of, ssem):
        def body(i):
            o = (me + i + 1) % E
            rc_(src_of(o), src_of(o), ssem.at[o], ssem.at[o], o, j).wait_send()

        loop(E - 1, body)

    class Tree:
        def __init__(self, buf, own, recv, sz, s2, s3, hook):
            self.buf, self.own, self.recv = buf, own, recv
            self.sz, self.s2, self.s3, self.hook = sz, s2, s3, hook

        def send(self, blk, ssem, chip, src=None):
            src = self.buf.at[blk] if src is None else src
            rc_(src, self.buf.at[blk], ssem, self.recv.at[blk], chip, j).start()

        def wait(self, blk):
            rc_(self.buf.at[blk], self.buf.at[blk], self.recv.at[blk], self.recv.at[blk], p2, j).wait_recv()

        def start(self):
            self.send(me, self.s3.at[0], p3, self.own)
            self.send(me, self.s2.at[0], p2, self.own)

            def body(i):
                self.send(me, self.sz.at[i], ((a + i + 1) % A) * 4 + r, self.own)

            loop(A - 1, body)
            self.hook(me, self.own)

        def stage_z(self):
            def body(i):
                blk = ((a + i + 1) % A) * 4 + r
                self.wait(blk)
                self.send(blk, self.s3.at[i + 1], p3)
                self.send(blk, self.s2.at[i + 1], p2)
                self.hook(blk, self.buf.at[blk])

            loop(A - 1, body)

        def stage_2(self):
            def body(i):
                blk = ((a + i) % A) * 4 + r2
                self.wait(blk)
                self.send(blk, self.s3.at[A + i], p3)
                self.hook(blk, self.buf.at[blk])

            loop(A, body)

        def stage_3(self):
            for rr in (r3, r23):
                def body(i):
                    blk = ((a + i) % A) * 4 + rr
                    self.wait(blk)
                    self.hook(blk, self.buf.at[blk])

                loop(A, body)

        def drain(self):
            def one(sem):
                rc_(self.own, self.own, sem, sem, p2, j).wait_send()

            loop(A - 1, lambda i: one(self.sz.at[i]))
            loop(A, lambda i: one(self.s2.at[i]))
            loop(2 * A, lambda i: one(self.s3.at[i]))

    def pair_hook(blk, src):
        if F > 1:
            for d in range(1, T):
                rc_(
                    src, gbuf.at[j, blk], g_ps.at[d, blk], g_pr.at[j, blk], me, (j + d) % T
                ).start()

    tree_g = Tree(gbuf.at[fj], own_g, g_recv, g_sz, g_s2, g_s3, pair_hook)
    tree_s = Tree(s3buf, s3buf.at[me], s3_recv, s3_sz, s3_s2, s3_s3, lambda blk, src: None)

    a2a_send(lambda o: x_ref.at[o], xbuf, x_s, x_r)
    tree_g.start()
    a2a_send(lambda o: m_ref, mbuf, m_s, m_r)
    xbuf[me] = x_ref[me]
    mbuf[me] = m_ref[...]
    gbuf[fj, me] = own_g[...]

    a2a_wait(xbuf, x_r)
    ps[...] = jnp.dot(flat(xbuf[...]), sd_ref[...], preferred_element_type=jnp.float32).astype(jnp.bfloat16).reshape(E, tok, FFl)
    a2a_send(lambda o: ps.at[o], s2buf, s2_s, s2_r)
    s2buf[me] = ps[me]

    tree_g.stage_z()

    a2a_wait(mbuf, m_r)
    meta = flat(mbuf[...])
    lane = lax.broadcasted_iota(jnp.int32, (tokens, LANES), 1)
    hit = jnp.where((meta == me.astype(jnp.float32)) & (lane < TOP), 1.0, 0.0)
    gates = pltpu.roll(meta, LANES - TOP, 1)
    chosen = jnp.sum(hit, axis=1, keepdims=True)
    gate = jnp.sum(hit * gates, axis=1, keepdims=True)
    wide = jnp.broadcast_to(chosen, (tokens, LANES))
    row = lax.broadcasted_iota(jnp.int32, (tokens, LANES), 0) % tok
    total = wide
    shift = 1
    while shift < tok:
        total = total + jnp.where(row >= shift, pltpu.roll(total, shift, 0), 0.0)
        shift *= 2
    position = (total - wide)[:, :1]
    slots = sr.shape[1]
    cap = slots // E
    base = (lax.broadcasted_iota(jnp.int32, (tokens, 1), 0) // tok) * cap
    target = position + base.astype(jnp.float32)
    slot = lax.broadcasted_iota(jnp.int32, (tokens, slots), 1).astype(jnp.float32)
    permute = jnp.where((slot == target) & (chosen > 0.5), 1.0, 0.0).astype(jnp.bfloat16)

    tree_g.stage_2()

    wcopies[0].wait()
    pre_gate = jnp.dot(permute, sr[0], preferred_element_type=jnp.float32)
    pre_up = jnp.dot(permute, sr[1], preferred_element_type=jnp.float32)
    sig = jax.nn.sigmoid(pre_gate)
    d_up = pre_gate * sig
    d_gate = pre_up * sig * (1.0 + pre_gate * (1.0 - sig))

    a2a_wait(s2buf, s2_r)
    shared_back = jnp.sum(s2buf[...].astype(jnp.float32), axis=0)
    sh = sv_ref[0].astype(jnp.float32)
    su = sv_ref[1].astype(jnp.float32)
    ssig = jax.nn.sigmoid(sh)
    s3buf[me, 0] = (shared_back * su * ssig * (1.0 + sh * (1.0 - ssig))).astype(jnp.bfloat16)
    s3buf[me, 1] = (shared_back * sh * ssig).astype(jnp.bfloat16)
    tree_s.start()

    tree_g.stage_3()
    tree_s.stage_z()

    wcopies[1].wait()
    if F > 1:
        back = jnp.zeros((tokens, FFl), jnp.float32)
        for d in range(1, T):
            other = (j + d) % T

            def body(i):
                ref = gbuf.at[other, i]
                rc_(ref, ref, g_pr.at[other, i], g_pr.at[other, i], me, other).wait_recv()

            loop(E, body)
        for t in range(F):
            back = back + dot_nt(flat(gbuf[t]), wd[:, t * H:(t + 1) * H])
    else:
        back = dot_nt(flat(gbuf[0]), wd[...])
    tree_s.stage_2()
    grad_up = back * d_up
    gate_sum = jnp.sum(grad_up * pre_up, axis=1, keepdims=True)
    gate_sum = gate_sum.astype(jnp.bfloat16).astype(jnp.float32)
    grad_gate = (back * d_gate * gate).astype(jnp.bfloat16)
    grad_up = (grad_up * gate).astype(jnp.bfloat16)
    gm[...] = jnp.where(lane == me, gate_sum, 0.0).reshape(E, tok, LANES)
    a2a_send(lambda o: gm.at[o], gmbuf, gm_s, gm_r)
    gmbuf[me] = gm[me]

    wcopies[2].wait()

    def rows_of(t, c):
        span = pl.ds(pl.multiple_of(t * HR + c * HC, 16), HC)
        return dot_nt(grad_gate, wgu[0, span, :]) + dot_nt(grad_up, wgu[1, span, :])

    for c in range(NC):
        for d in range(1, T):
            t = (j + d) % T
            pairsend[d - 1, c] = rows_of(t, c).astype(jnp.bfloat16)
            rc_(
                pairsend.at[d - 1, c], pairbuf.at[T - 1 - d, c],
                pair_s.at[d - 1, c], pair_r.at[T - 1 - d, c], me, t,
            ).start()

    def stage3_blocks(c, i):
        ap = i // 2
        w = i % 2
        blk = ap * 4 + r3 * (1 - w) + r23 * w
        return rc_(part.at[c, blk], r3buf.at[c, i], r3_s.at[c, i], r3_r.at[c, i], p3, j)

    for c in range(NC):
        mine = rows_of(j, c)
        for d in range(1, T):
            rc_(
                pairsend.at[d - 1, c], pairbuf.at[d - 1, c],
                pair_s.at[d - 1, c], pair_r.at[d - 1, c], me, (j + d) % T,
            ).wait_recv()
            mine = mine + pairbuf[d - 1, c].astype(jnp.float32)
        part[c] = mine.astype(jnp.bfloat16).reshape(E, tok, HC)
        loop(2 * A, lambda i: stage3_blocks(c, i).start())

    tree_s.stage_3()
    term = dot_nt(flat(s3buf[:, 0]), sgu_ref[0]) + dot_nt(flat(s3buf[:, 1]), sgu_ref[1])
    st[...] = term.astype(jnp.bfloat16).reshape(E, tok, st.shape[2])
    a2a_send(lambda o: st.at[o], s4buf, s4_s, s4_r)
    s4buf[me] = st[me]

    def stage2_block(c, i):
        return rc_(part.at[c, i * 4 + r2], r2buf.at[c, i], r2_s.at[c, i], r2_r.at[c, i], p2, j)

    for c in range(NC):
        loop(2 * A, lambda i: stage3_blocks(c, i).wait_recv())

        def add_first(i):
            blk = i * 4 + r2
            part[c, blk] = (
                part[c, blk].astype(jnp.float32) + r3buf[c, i * 2 + 1].astype(jnp.float32)
            ).astype(jnp.bfloat16)

        loop(A, add_first)
        loop(A, lambda i: stage2_block(c, i).start())

    def stagez_block(c, i):
        o = (a + i + 1) % A
        return rc_(
            part.at[c, o * 4 + r], rzbuf.at[c, a], rz_s.at[c, o], rz_r.at[c, a], o * 4 + r, j
        )

    for c in range(NC):
        loop(A, lambda i: stage2_block(c, i).wait_recv())

        def add_second(i):
            blk = i * 4 + r
            part[c, blk] = (
                part[c, blk].astype(jnp.float32)
                + r3buf[c, i * 2].astype(jnp.float32)
                + r2buf[c, i].astype(jnp.float32)
            ).astype(jnp.bfloat16)

        loop(A, add_second)
        loop(A - 1, lambda i: stagez_block(c, i).start())
        rzbuf[c, a] = part[c, me]

    a2a_wait(gmbuf, gm_r)
    gpair[T - 1] = jnp.sum(gmbuf[...], axis=0)
    a2a_wait(s4buf, s4_r)
    group = E // T
    for d in range(1, T):
        t = (j + d) % T
        rc_(gpair.at[T - 1], gpair.at[T - 1 - d], gp_s.at[d - 1], gp_r.at[T - 1 - d], me, t).start()
        rc_(
            s4buf.at[pl.ds(t * group, group)], s4pair.at[T - 1 - d],
            s4p_s.at[d - 1], s4p_r.at[T - 1 - d], me, t,
        ).start()
    shared = s4buf[pl.ds(j * group, group)].astype(jnp.float32)
    for d in range(1, T):
        rc_(gpair.at[T - 1], gpair.at[d - 1], gp_s.at[d - 1], gp_r.at[d - 1], me, (j + d) % T).wait_recv()
        rc_(
            s4pair.at[d - 1], s4pair.at[d - 1], s4p_s.at[d - 1], s4p_r.at[d - 1], me, (j + d) % T
        ).wait_recv()
        shared = shared + s4pair[d - 1].astype(jnp.float32)
    for o in range(group):
        spread[:, o * DS:(o + 1) * DS] = shared[o]
    sums = jnp.sum(gpair[...], axis=0)
    own_meta = m_ref[...]
    lane16 = lax.broadcasted_iota(jnp.int32, (tok, LANES), 1)
    lane_f = lane16.astype(jnp.float32)
    result = jnp.zeros((tok, LANES), jnp.float32)
    for k in range(TOP):
        value = jnp.sum(
            jnp.where(lane_f == own_meta[:, k:k + 1], sums, 0.0), axis=1, keepdims=True
        )
        result = jnp.where(lane16 == k, value, result)
    square[0:tok] = result
    out_g[...] = square[...].T[0:TOP, 0:tok]

    for c in range(NC):
        def wait_z(i):
            o = (a + i + 1) % A
            rc_(rzbuf.at[c, o], rzbuf.at[c, o], rz_s.at[c, o], rz_r.at[c, o], p2, j).wait_recv()

        loop(A - 1, wait_z)
        span = slice(c * HC, (c + 1) * HC)
        out_r[:, span] = (
            jnp.sum(rzbuf[c].astype(jnp.float32), axis=0) + spread[:, span]
        ).astype(jnp.bfloat16)

    a2a_drain(lambda o: x_ref.at[o], x_s)
    a2a_drain(lambda o: m_ref, m_s)
    a2a_drain(lambda o: ps.at[o], s2_s)
    a2a_drain(lambda o: gm.at[o], gm_s)
    a2a_drain(lambda o: st.at[o], s4_s)
    tree_g.drain()
    tree_s.drain()
    for d in range(1, T):
        if F > 1:
            loop(
                E,
                lambda i: rc_(
                    gbuf.at[j, i], gbuf.at[j, i], g_ps.at[d, i], g_ps.at[d, i], me, (j + d) % T
                ).wait_send(),
            )
        rc_(gpair.at[T - 1], gpair.at[T - 1], gp_s.at[d - 1], gp_s.at[d - 1], me, (j + d) % T).wait_send()
        rc_(
            s4pair.at[d - 1], s4pair.at[d - 1], s4p_s.at[d - 1], s4p_s.at[d - 1], me, (j + d) % T
        ).wait_send()
        for c in range(NC):
            ref = pairsend.at[d - 1, c]
            rc_(ref, ref, pair_s.at[d - 1, c], pair_s.at[d - 1, c], me, (j + d) % T).wait_send()
    for c in range(NC):
        loop(2 * A, lambda i: stage3_blocks(c, i).wait_send())
        loop(A, lambda i: stage2_block(c, i).wait_send())
        loop(A - 1, lambda i: stagez_block(c, i).wait_send())


def per_device(
    E, T,
    grad_out, expert_ids, gate_values, w_gate_up, w_down, saved_routed,
    shared_gate_up, shared_down, saved_shared,
):
    tok, D = grad_out.shape
    TOP = expert_ids.shape[1]
    FFl = w_down.shape[1]
    DS = shared_down.shape[1]
    slots = saved_routed.shape[2]
    F = T if (D // T) % LANES == 0 else 1
    H = D // F
    HR = D // T
    NC = 2 if HR % (2 * LANES) == 0 else 1
    HC = HR // NC
    A = E // 4
    tokens = E * tok
    bf, f32 = jnp.bfloat16, jnp.float32
    V, S = pltpu.VMEM, pltpu.SemaphoreType.DMA
    T1 = max(T - 1, 1)
    scratch = [
        V((E, tok, DS), bf), V((tok, LANES), f32), V((LANES, LANES), f32), V((tok, HR), f32),
        V((F, E, tok, H), bf), V((E, tok, DS), bf), V((E, tok, LANES), f32),
        V((FFl, D), bf), V((2, D, FFl), bf), V((2, slots, FFl), bf),
        V((E, tok, FFl), bf), V((E, tok, FFl), bf), V((E, 2, tok, FFl), bf),
        V((E, tok, DS), bf), V((E, tok, DS), bf), V((T1, E // T, tok, DS), bf),
        V((E, tok, LANES), f32), V((E, tok, LANES), f32), V((T, tok, LANES), f32),
        V((T1, NC, tokens, HC), bf), V((T1, NC, tokens, HC), bf), V((NC, E, tok, HC), bf),
        V((NC, 2 * A, tok, HC), bf), V((NC, A, tok, HC), bf), V((NC, A, tok, HC), bf),
        S((3,)), S((E,)), S((A,)), S((A,)), S((2 * A,)), S((T, E)), S((T, E)),
        S((E,)), S((A,)), S((A,)), S((2 * A,)),
        S((E,)), S((E,)), S((E,)), S((E,)), S((E,)), S((E,)), S((E,)), S((E,)), S((E,)), S((E,)),
        S((T1,)), S((T1,)), S((T1,)), S((T1,)), S((T1, NC)), S((T1, NC)),
        S((NC, 2 * A)), S((NC, 2 * A)), S((NC, A)), S((NC, A)), S((NC, A)), S((NC, A)),
    ]
    vm = pl.BlockSpec(memory_space=pltpu.VMEM)
    hbm = pl.BlockSpec(memory_space=pltpu.HBM)
    grad_in, gates = pl.pallas_call(
        functools.partial(kernel, E, T, F, NC, TOP),
        out_shape=(
            jax.ShapeDtypeStruct((tok, HR), bf),
            jax.ShapeDtypeStruct((TOP, tok), f32),
        ),
        in_specs=[vm] * 6 + [hbm] * 3,
        out_specs=(vm, vm),
        scratch_shapes=scratch,
        compiler_params=pltpu.CompilerParams(
            collective_id=0, has_side_effects=True, vmem_limit_bytes=60 * 1024 * 1024
        ),
    )(
        grad_out, expert_ids.T, gate_values.T, saved_shared, shared_gate_up, shared_down.T,
        w_down[0], w_gate_up[0], saved_routed[0],
    )
    return grad_in, gates.T


def solution(mesh):
    return jax.shard_map(
        functools.partial(per_device, mesh.shape["expert"], mesh.shape["tensor"]),
        mesh=mesh,
        in_specs=(
            P("expert", None),
            P("expert", None),
            P("expert", None),
            P("expert", None, None, "tensor"),
            P("expert", "tensor", None),
            P("expert", None, None, "tensor"),
            P(None, "expert", "tensor"),
            P("tensor", "expert"),
            P(None, "expert", "tensor"),
        ),
        out_specs=(P("expert", "tensor"), P("expert", None)),
        check_vma=False,
    )
```

```python
import functools

import jax
import jax.numpy as jnp
from jax import lax
from jax.experimental import pallas as pl
from jax.experimental.pallas import tpu as pltpu
from jax.sharding import PartitionSpec as P

MESH = pl.DeviceIdType.MESH
LANES = 128


def dot_nt(left, right):
    return lax.dot_general(
        left, right, (((1,), (1,)), ((), ())), preferred_element_type=jnp.float32
    )


def loop(count, body):
    def step(i, carry):
        body(i)
        return carry

    lax.fori_loop(0, count, step, 0)


def flat(value):
    return value.reshape(-1, value.shape[-1])


def kernel(
    E, T, F, NC, TOP,
    g_ref, id_ref, gv_ref, sv_ref, sd_hbm, sr_hbm, wd_hbm, sgu_hbm, wgu_hbm,
    out_r, out_g,
    x_ref, square, spread, gbuf, xbuf, sd, sr, wd, sgu, wgu,
    ps, q3buf, q2buf, qzbuf, s3buf, st, s4buf, s4pair,
    pairsend, pairbuf, part, r3buf, r2buf, rzbuf,
    wsem, g_recv, g_sz, g_s2, g_s3, g_ps, g_pr,
    s3_recv, s3_sz, s3_s2, s3_s3,
    x_s, x_r, s4_s, s4_r, s4p_s, s4p_r, pair_s, pair_r,
    r3_s, r3_r, r2_s, r2_r, rz_s, rz_r,
    q3_s, q3_r, q2_s, q2_r, qz_s, qz_r,
):
    me = lax.axis_index("expert")
    j = lax.axis_index("tensor")
    A = E // 4
    a = me // 4
    r = me % 4
    rc = r + 1 - 2 * (r % 2)
    rb = r + 2 - 4 * (r // 2)
    odd = j % 2
    r2 = rc * (1 - odd) + rb * odd
    r3 = rb * (1 - odd) + rc * odd
    r23 = 3 - r
    p2 = a * 4 + r2
    p3 = a * 4 + r3
    fj = j if F > 1 else 0
    tok = x_ref.shape[1]
    DS = x_ref.shape[2]
    FFl = wd.shape[0]
    H = gbuf.shape[3] - LANES
    own_g = gbuf.at[fj, me]
    HC = part.shape[3] - LANES
    HR = HC * NC
    tokens = E * tok

    def rc_(src, dst, ssem, rsem, chip, core):
        return pltpu.make_async_remote_copy(
            src_ref=src, dst_ref=dst, send_sem=ssem, recv_sem=rsem,
            device_id=(chip, core), device_id_type=MESH,
        )

    wcopies = [
        pltpu.make_async_copy(sd_hbm, sd, wsem.at[0]),
        pltpu.make_async_copy(sr_hbm, sr, wsem.at[1]),
        pltpu.make_async_copy(wd_hbm, wd, wsem.at[2]),
        pltpu.make_async_copy(sgu_hbm, sgu, wsem.at[3]),
        pltpu.make_async_copy(wgu_hbm, wgu, wsem.at[4]),
    ]
    for copy in wcopies:
        copy.start()

    barrier = pltpu.get_barrier_semaphore()

    def greet(i):
        pl.semaphore_signal(barrier, inc=1, device_id=((me + i + 1) % E, j), device_id_type=MESH)

    loop(E - 1, greet)
    for d in range(1, T):
        pl.semaphore_signal(barrier, inc=1, device_id=(me, (j + d) % T), device_id_type=MESH)

    for o in range(E):
        x_ref[o] = g_ref[:, o * DS:(o + 1) * DS]
    square[...] = jnp.zeros_like(square)
    square[0:TOP, 0:tok] = id_ref[...].astype(jnp.float32)
    high = gv_ref[...].astype(jnp.bfloat16).astype(jnp.float32)
    square[TOP:2 * TOP, 0:tok] = high
    square[2 * TOP:3 * TOP, 0:tok] = gv_ref[...] - high
    own_meta = square[...].T[0:tok]
    gbuf[fj, me, :, 0:LANES] = own_meta.astype(jnp.bfloat16)
    if F > 1:
        gbuf[fj, me, :, LANES:] = g_ref[:, pl.ds(pl.multiple_of(fj * H, LANES), H)]
    else:
        gbuf[fj, me, :, LANES:] = g_ref[...]

    pl.semaphore_wait(barrier, E - 1 + T - 1)

    def a2a_send(src_of, dst, ssem, rsem):
        def body(i):
            o = (me + i + 1) % E
            rc_(src_of(o), dst.at[me], ssem.at[o], rsem.at[me], o, j).start()

        loop(E - 1, body)

    def a2a_wait(dst, rsem):
        def body(i):
            o = (me + i + 1) % E
            rc_(dst.at[o], dst.at[o], rsem.at[o], rsem.at[o], o, j).wait_recv()

        loop(E - 1, body)

    def a2a_drain(src_of, ssem):
        def body(i):
            o = (me + i + 1) % E
            rc_(src_of(o), src_of(o), ssem.at[o], ssem.at[o], o, j).wait_send()

        loop(E - 1, body)

    class Tree:
        def __init__(self, buf, own, recv, sz, s2, s3, hook):
            self.buf, self.own, self.recv = buf, own, recv
            self.sz, self.s2, self.s3, self.hook = sz, s2, s3, hook

        def send(self, blk, ssem, chip, src=None):
            src = self.buf.at[blk] if src is None else src
            rc_(src, self.buf.at[blk], ssem, self.recv.at[blk], chip, j).start()

        def wait(self, blk):
            rc_(self.buf.at[blk], self.buf.at[blk], self.recv.at[blk], self.recv.at[blk], p2, j).wait_recv()

        def start(self):
            self.send(me, self.s3.at[0], p3, self.own)
            self.send(me, self.s2.at[0], p2, self.own)

            def body(i):
                self.send(me, self.sz.at[i], ((a + i + 1) % A) * 4 + r, self.own)

            loop(A - 1, body)
            self.hook(me, self.own)

        def stage_z(self):
            def body(i):
                blk = ((a + i + 1) % A) * 4 + r
                self.wait(blk)
                self.send(blk, self.s3.at[i + 1], p3)
                self.send(blk, self.s2.at[i + 1], p2)
                self.hook(blk, self.buf.at[blk])

            loop(A - 1, body)

        def stage_2(self):
            def body(i):
                blk = ((a + i) % A) * 4 + r2
                self.wait(blk)
                self.send(blk, self.s3.at[A + i], p3)
                self.hook(blk, self.buf.at[blk])

            loop(A, body)

        def stage_3(self):
            for rr in (r3, r23):
                def body(i):
                    blk = ((a + i) % A) * 4 + rr
                    self.wait(blk)
                    self.hook(blk, self.buf.at[blk])

                loop(A, body)

        def drain(self):
            def one(sem):
                rc_(self.own, self.own, sem, sem, p2, j).wait_send()

            loop(A - 1, lambda i: one(self.sz.at[i]))
            loop(A, lambda i: one(self.s2.at[i]))
            loop(2 * A, lambda i: one(self.s3.at[i]))

    class Reduce:
        def __init__(self, part, b3, b2, bz, s3, v3, s2, v2, sz, vz):
            self.part, self.b3, self.b2, self.bz = part, b3, b2, bz
            self.s3, self.v3, self.s2, self.v2, self.sz, self.vz = s3, v3, s2, v2, sz, vz

        def copy3(self, i):
            first = 1 - i // A
            blk = (i % A) * 4 + r23 * first + r3 * (1 - first)
            return rc_(self.part.at[blk], self.b3.at[i], self.s3.at[i], self.v3.at[i], p3, j)

        def copy2(self, i):
            return rc_(self.part.at[i * 4 + r2], self.b2.at[i], self.s2.at[i], self.v2.at[i], p2, j)

        def copyz(self, o):
            return rc_(
                self.part.at[o * 4 + r], self.bz.at[a], self.sz.at[o], self.vz.at[a], o * 4 + r, j
            )

        def start(self):
            loop(2 * A, lambda i: self.copy3(i).start())

        def stage_2(self):
            def body(i):
                self.copy3(i).wait_recv()
                blk = i * 4 + r2
                self.part[blk] = (
                    self.part[blk].astype(jnp.float32) + self.b3[i].astype(jnp.float32)
                ).astype(jnp.bfloat16)
                self.copy2(i).start()

            loop(A, body)

        def stage_z(self):
            def total(o):
                self.copy3(A + o).wait_recv()
                self.copy2(o).wait_recv()
                return (
                    self.part[o * 4 + r].astype(jnp.float32)
                    + self.b3[A + o].astype(jnp.float32)
                    + self.b2[o].astype(jnp.float32)
                ).astype(jnp.bfloat16)

            def body(i):
                o = (a + i + 1) % A
                self.part[o * 4 + r] = total(o)
                self.copyz(o).start()

            loop(A - 1, body)
            self.bz[a] = total(a)

        def finish(self):
            def body(i):
                o = (a + i + 1) % A
                rc_(self.bz.at[o], self.bz.at[o], self.sz.at[o], self.vz.at[o], p2, j).wait_recv()

            loop(A - 1, body)
            out = self.bz[0].astype(jnp.float32)
            for i in range(1, A):
                out = out + self.bz[i].astype(jnp.float32)
            return out

        def drain(self):
            loop(2 * A, lambda i: self.copy3(i).wait_send())
            loop(A, lambda i: self.copy2(i).wait_send())
            loop(A - 1, lambda i: self.copyz((a + i + 1) % A).wait_send())

    def pair_hook(blk, src):
        if F > 1:
            for d in range(1, T):
                rc_(
                    src, gbuf.at[j, blk], g_ps.at[d, blk], g_pr.at[j, blk], me, (j + d) % T
                ).start()

    tree_g = Tree(gbuf.at[fj], own_g, g_recv, g_sz, g_s2, g_s3, pair_hook)
    tree_s = Tree(s3buf, s3buf.at[me], s3_recv, s3_sz, s3_s2, s3_s3, lambda blk, src: None)

    red_q = Reduce(ps, q3buf, q2buf, qzbuf, q3_s, q3_r, q2_s, q2_r, qz_s, qz_r)
    red_r = []
    for c in range(NC):
        cols = pl.ds(0, LANES + HC) if c == 0 else pl.ds(LANES, HC)
        red_r.append(
            Reduce(
                part.at[c, :, :, cols], r3buf.at[c, :, :, cols], r2buf.at[c, :, :, cols],
                rzbuf.at[c, :, :, cols], r3_s.at[c], r3_r.at[c], r2_s.at[c], r2_r.at[c],
                rz_s.at[c], rz_r.at[c],
            )
        )

    a2a_send(lambda o: x_ref.at[o], xbuf, x_s, x_r)
    tree_g.start()
    xbuf[me] = x_ref[me]

    wcopies[0].wait()
    a2a_wait(xbuf, x_r)
    partial = jnp.dot(flat(xbuf[...]), sd[...], preferred_element_type=jnp.float32)
    ps[...] = partial.astype(jnp.bfloat16).reshape(E, tok, FFl)
    red_q.start()

    tree_g.stage_z()
    red_q.stage_2()
    tree_g.stage_2()
    red_q.stage_z()
    tree_g.stage_3()

    shared_back = red_q.finish()
    sh = sv_ref[0].astype(jnp.float32)
    su = sv_ref[1].astype(jnp.float32)
    ssig = jax.nn.sigmoid(sh)
    s3buf[me, 0] = (shared_back * su * ssig * (1.0 + sh * (1.0 - ssig))).astype(jnp.bfloat16)
    s3buf[me, 1] = (shared_back * sh * ssig).astype(jnp.bfloat16)
    tree_s.start()

    meta = flat(gbuf[fj, :, :, 0:LANES]).astype(jnp.float32)
    lane = lax.broadcasted_iota(jnp.int32, (tokens, LANES), 1)
    hit = jnp.where((meta == me.astype(jnp.float32)) & (lane < TOP), 1.0, 0.0)
    gates = pltpu.roll(meta, LANES - TOP, 1) + pltpu.roll(meta, LANES - 2 * TOP, 1)
    chosen = jnp.sum(hit, axis=1, keepdims=True)
    gate = jnp.sum(hit * gates, axis=1, keepdims=True)
    wide = jnp.broadcast_to(chosen, (tokens, LANES))
    row = lax.broadcasted_iota(jnp.int32, (tokens, LANES), 0) % tok
    total = wide
    shift = 1
    while shift < tok:
        total = total + jnp.where(row >= shift, pltpu.roll(total, shift, 0), 0.0)
        shift *= 2
    position = (total - wide)[:, :1]
    slots = sr.shape[1]
    cap = slots // E
    base = (lax.broadcasted_iota(jnp.int32, (tokens, 1), 0) // tok) * cap
    target = position + base.astype(jnp.float32)
    slot = lax.broadcasted_iota(jnp.int32, (tokens, slots), 1).astype(jnp.float32)
    permute = jnp.where((slot == target) & (chosen > 0.5), 1.0, 0.0).astype(jnp.bfloat16)
    wcopies[1].wait()
    pre_gate = jnp.dot(permute, sr[0], preferred_element_type=jnp.float32)
    pre_up = jnp.dot(permute, sr[1], preferred_element_type=jnp.float32)
    sig = jax.nn.sigmoid(pre_gate)
    d_up = pre_gate * sig
    d_gate = pre_up * sig * (1.0 + pre_gate * (1.0 - sig))

    wcopies[2].wait()

    def back_of(t):
        return dot_nt(flat(gbuf[t, :, :, LANES:]), wd[:, pl.ds(pl.multiple_of(t * H, LANES), H)])

    if F > 1:
        back = back_of(j)
        for d in range(1, T):
            other = (j + d) % T

            def body(i):
                ref = gbuf.at[other, i]
                rc_(ref, ref, g_pr.at[other, i], g_pr.at[other, i], me, other).wait_recv()

            loop(E, body)
            back = back + back_of(other)
    else:
        back = dot_nt(flat(gbuf[0, :, :, LANES:]), wd[...])
    tree_s.stage_z()
    grad_up = back * d_up
    gate_sum = jnp.sum(grad_up * pre_up, axis=1, keepdims=True)
    grad_gate = (back * d_gate * gate).astype(jnp.bfloat16)
    grad_up = (grad_up * gate).astype(jnp.bfloat16)
    place = j * E + me if T * E <= LANES else me
    gate_row = jnp.where(lane == place, gate_sum, 0.0).astype(jnp.bfloat16)

    wcopies[4].wait()

    def rows_of(t, c):
        span = pl.ds(pl.multiple_of(t * HR + c * HC, 16), HC)
        return dot_nt(grad_gate, wgu[0, span, :]) + dot_nt(grad_up, wgu[1, span, :])

    for c in range(NC):
        for d in range(1, T):
            t = (j + d) % T
            pairsend[d - 1, c, :, LANES:] = rows_of(t, c).astype(jnp.bfloat16)
            if c == 0:
                pairsend[d - 1, c, :, 0:LANES] = gate_row
            rc_(
                pairsend.at[d - 1, c], pairbuf.at[T - 1 - d, c],
                pair_s.at[d - 1, c], pair_r.at[T - 1 - d, c], me, t,
            ).start()

    tree_s.stage_2()

    for c in range(NC):
        mine = rows_of(j, c)
        for d in range(1, T):
            rc_(
                pairsend.at[d - 1, c], pairbuf.at[d - 1, c],
                pair_s.at[d - 1, c], pair_r.at[d - 1, c], me, (j + d) % T,
            ).wait_recv()
            mine = mine + pairbuf[d - 1, c, :, LANES:].astype(jnp.float32)
        part[c, :, :, LANES:] = mine.astype(jnp.bfloat16).reshape(E, tok, HC)
        if c == 0:
            sums = gate_row.astype(jnp.float32)
            for d in range(1, T):
                sums = sums + pairbuf[d - 1, c, :, 0:LANES].astype(jnp.float32)
            part[c, :, :, 0:LANES] = sums.astype(jnp.bfloat16).reshape(E, tok, LANES)
        red_r[c].start()

    tree_s.stage_3()
    wcopies[3].wait()
    term = dot_nt(flat(s3buf[:, 0]), sgu[0]) + dot_nt(flat(s3buf[:, 1]), sgu[1])
    st[...] = term.astype(jnp.bfloat16).reshape(E, tok, st.shape[2])
    a2a_send(lambda o: st.at[o], s4buf, s4_s, s4_r)
    s4buf[me] = st[me]

    a2a_drain(lambda o: x_ref.at[o], x_s)
    tree_g.drain()
    red_q.drain()
    if F > 1:
        for d in range(1, T):
            loop(
                E,
                lambda i: rc_(
                    gbuf.at[j, i], gbuf.at[j, i], g_ps.at[d, i], g_ps.at[d, i], me, (j + d) % T
                ).wait_send(),
            )

    for c in range(NC):
        red_r[c].stage_2()
        red_r[c].stage_z()
    tree_s.drain()

    a2a_wait(s4buf, s4_r)
    group = E // T
    for d in range(1, T):
        t = (j + d) % T
        rc_(
            s4buf.at[pl.ds(t * group, group)], s4pair.at[T - 1 - d],
            s4p_s.at[d - 1], s4p_r.at[T - 1 - d], me, t,
        ).start()
    shared = s4buf[pl.ds(j * group, group)].astype(jnp.float32)
    for d in range(1, T):
        rc_(
            s4pair.at[d - 1], s4pair.at[d - 1], s4p_s.at[d - 1], s4p_r.at[d - 1], me, (j + d) % T
        ).wait_recv()
        shared = shared + s4pair[d - 1].astype(jnp.float32)
    for o in range(group):
        spread[:, o * DS:(o + 1) * DS] = shared[o]
    a2a_drain(lambda o: st.at[o], s4_s)
    for d in range(1, T):
        rc_(
            s4pair.at[d - 1], s4pair.at[d - 1], s4p_s.at[d - 1], s4p_s.at[d - 1], me, (j + d) % T
        ).wait_send()
        for c in range(NC):
            ref = pairsend.at[d - 1, c]
            rc_(ref, ref, pair_s.at[d - 1, c], pair_s.at[d - 1, c], me, (j + d) % T).wait_send()

    done = [red_r[c].finish() for c in range(NC)]
    for c in range(NC):
        rows = done[c][:, LANES:] if c == 0 else done[c]
        out_r[:, c * HC:(c + 1) * HC] = rows + spread[:, c * HC:(c + 1) * HC]
    sums = done[0][:, 0:LANES]
    lane16 = lax.broadcasted_iota(jnp.int32, (tok, LANES), 1)
    expert_f = (lane16 % E).astype(jnp.float32)
    for parity in range(2):
        some = jnp.where(lane16 % 2 == parity, sums, 0.0)
        result = jnp.zeros((tok, LANES), jnp.float32)
        for k in range(TOP):
            value = jnp.sum(
                jnp.where(expert_f == own_meta[:, k:k + 1], some, 0.0), axis=1, keepdims=True
            )
            result = jnp.where(lane16 == k, value, result)
        square[0:tok] = result
        out_g[parity] = square[...].T[0:TOP, 0:tok]
    for c in range(NC):
        red_r[c].drain()


def per_device(
    E, T,
    grad_out, expert_ids, gate_values, w_gate_up, w_down, saved_routed,
    shared_gate_up, shared_down, saved_shared,
):
    tok, D = grad_out.shape
    TOP = expert_ids.shape[1]
    FFl = w_down.shape[1]
    DS = shared_down.shape[1]
    slots = saved_routed.shape[2]
    F = T if (D // T) % LANES == 0 else 1
    H = D // F
    HR = D // T
    NC = 2 if HR % (2 * LANES) == 0 else 1
    HC = HR // NC
    A = E // 4
    tokens = E * tok
    bf, f32 = jnp.bfloat16, jnp.float32
    V, S = pltpu.VMEM, pltpu.SemaphoreType.DMA
    T1 = max(T - 1, 1)
    W = LANES + HC
    scratch = [
        V((E, tok, DS), bf), V((LANES, LANES), f32), V((tok, HR), f32),
        V((F, E, tok, LANES + H), bf), V((E, tok, DS), bf),
        V((DS, FFl), bf), V((2, slots, FFl), bf), V((FFl, D), bf), V((2, DS, FFl), bf), V((2, D, FFl), bf),
        V((E, tok, FFl), bf), V((2 * A, tok, FFl), bf), V((A, tok, FFl), bf), V((A, tok, FFl), bf),
        V((E, 2, tok, FFl), bf),
        V((E, tok, DS), bf), V((E, tok, DS), bf), V((T1, E // T, tok, DS), bf),
        V((T1, NC, tokens, W), bf), V((T1, NC, tokens, W), bf), V((NC, E, tok, W), bf),
        V((NC, 2 * A, tok, W), bf), V((NC, A, tok, W), bf), V((NC, A, tok, W), bf),
        S((5,)), S((E,)), S((A,)), S((A,)), S((2 * A,)), S((T, E)), S((T, E)),
        S((E,)), S((A,)), S((A,)), S((2 * A,)),
        S((E,)), S((E,)), S((E,)), S((E,)), S((T1,)), S((T1,)), S((T1, NC)), S((T1, NC)),
        S((NC, 2 * A)), S((NC, 2 * A)), S((NC, A)), S((NC, A)), S((NC, A)), S((NC, A)),
        S((2 * A,)), S((2 * A,)), S((A,)), S((A,)), S((A,)), S((A,)),
    ]
    vm = pl.BlockSpec(memory_space=pltpu.VMEM)
    hbm = pl.BlockSpec(memory_space=pltpu.HBM)
    grad_in, gates = pl.pallas_call(
        functools.partial(kernel, E, T, F, NC, TOP),
        out_shape=(
            jax.ShapeDtypeStruct((tok, HR), f32),
            jax.ShapeDtypeStruct((2, TOP, tok), f32),
        ),
        in_specs=[vm] * 4 + [hbm] * 5,
        out_specs=(vm, vm),
        scratch_shapes=scratch,
        compiler_params=pltpu.CompilerParams(
            collective_id=0, has_side_effects=True, vmem_limit_bytes=60 * 1024 * 1024
        ),
    )(
        grad_out, expert_ids.T, gate_values.T, saved_shared, shared_down.T, saved_routed[0],
        w_down[0], shared_gate_up, w_gate_up[0],
    )
    return grad_in.astype(bf), (gates[0] + gates[1]).T


def solution(mesh):
    return jax.shard_map(
        functools.partial(per_device, mesh.shape["expert"], mesh.shape["tensor"]),
        mesh=mesh,
        in_specs=(
            P("expert", None),
            P("expert", None),
            P("expert", None),
            P("expert", None, None, "tensor"),
            P("expert", "tensor", None),
            P("expert", None, None, "tensor"),
            P(None, "expert", "tensor"),
            P("tensor", "expert"),
            P(None, "expert", "tensor"),
        ),
        out_specs=(P("expert", "tensor"), P("expert", None)),
        check_vma=False,
    )
```

```python
import functools

import jax
import jax.numpy as jnp
from jax import lax
from jax.experimental import pallas as pl
from jax.experimental.pallas import tpu as pltpu
from jax.sharding import PartitionSpec as P

MESH = pl.DeviceIdType.MESH
LANES = 128


def dot_nt(left, right):
    return lax.dot_general(
        left, right, (((1,), (1,)), ((), ())), preferred_element_type=jnp.float32
    )


def loop(count, body):
    def step(i, carry):
        body(i)
        return carry

    lax.fori_loop(0, count, step, 0)


def flat(value):
    return value.reshape(-1, value.shape[-1])


def kernel(
    E, T, F, NC, TOP,
    g_ref, id_ref, gv_ref, sv_ref, sd_hbm, sr_hbm, wd_hbm, sgu_hbm, wgu_hbm,
    out_r, out_g,
    square, spread, gbuf, sd, sdpad, sr, wd, sgu, wgu,
    ps, q3buf, q2buf, qzbuf, s3buf, st, s4buf, s4pair,
    pairsend, pairbuf, part, r3buf, r2buf, rzbuf,
    wsem, g_recv, g_sz, g_s2, g_s3, g_ps, g_pr,
    s3_recv, s3_sz, s3_s2, s3_s3,
    s4_s, s4_r, s4p_s, s4p_r, pair_s, pair_r,
    r3_s, r3_r, r2_s, r2_r, rz_s, rz_r,
    q3_s, q3_r, q2_s, q2_r, qz_s, qz_r,
):
    me = lax.axis_index("expert")
    j = lax.axis_index("tensor")
    A = E // 4
    a = me // 4
    r = me % 4
    rc = r + 1 - 2 * (r % 2)
    rb = r + 2 - 4 * (r // 2)
    odd = j % 2
    r2 = rc * (1 - odd) + rb * odd
    r3 = rb * (1 - odd) + rc * odd
    r23 = 3 - r
    p2 = a * 4 + r2
    p3 = a * 4 + r3
    fj = j if F > 1 else 0
    tok = g_ref.shape[0]
    DS = sd.shape[0]
    FFl = wd.shape[0]
    H = gbuf.shape[3] - LANES
    own_g = gbuf.at[fj, me]
    HC = part.shape[3] - LANES
    HR = HC * NC
    tokens = E * tok

    def rc_(src, dst, ssem, rsem, chip, core):
        return pltpu.make_async_remote_copy(
            src_ref=src, dst_ref=dst, send_sem=ssem, recv_sem=rsem,
            device_id=(chip, core), device_id_type=MESH,
        )

    wcopies = [
        pltpu.make_async_copy(sd_hbm, sd, wsem.at[0]),
        pltpu.make_async_copy(sr_hbm, sr, wsem.at[1]),
        pltpu.make_async_copy(wd_hbm, wd, wsem.at[2]),
        pltpu.make_async_copy(sgu_hbm, sgu, wsem.at[3]),
        pltpu.make_async_copy(wgu_hbm, wgu, wsem.at[4]),
    ]
    for copy in wcopies:
        copy.start()

    barrier = pltpu.get_barrier_semaphore()

    def greet(i):
        pl.semaphore_signal(barrier, inc=1, device_id=((me + i + 1) % E, j), device_id_type=MESH)

    loop(E - 1, greet)
    for d in range(1, T):
        pl.semaphore_signal(barrier, inc=1, device_id=(me, (j + d) % T), device_id_type=MESH)

    sdpad[...] = jnp.zeros_like(sdpad)
    square[...] = jnp.zeros_like(square)
    square[0:TOP, 0:tok] = id_ref[...].astype(jnp.float32)
    high = gv_ref[...].astype(jnp.bfloat16).astype(jnp.float32)
    square[TOP:2 * TOP, 0:tok] = high
    square[2 * TOP:3 * TOP, 0:tok] = gv_ref[...] - high
    own_meta = square[...].T[0:tok]
    gbuf[fj, me, :, 0:LANES] = own_meta.astype(jnp.bfloat16)
    if F > 1:
        gbuf[fj, me, :, LANES:] = g_ref[:, pl.ds(pl.multiple_of(fj * H, LANES), H)]
    else:
        gbuf[fj, me, :, LANES:] = g_ref[...]

    pl.semaphore_wait(barrier, E - 1 + T - 1)

    def a2a_send(src_of, dst, ssem, rsem):
        def body(i):
            o = (me + i + 1) % E
            rc_(src_of(o), dst.at[me], ssem.at[o], rsem.at[me], o, j).start()

        loop(E - 1, body)

    def a2a_wait(dst, rsem):
        def body(i):
            o = (me + i + 1) % E
            rc_(dst.at[o], dst.at[o], rsem.at[o], rsem.at[o], o, j).wait_recv()

        loop(E - 1, body)

    def a2a_drain(src_of, ssem):
        def body(i):
            o = (me + i + 1) % E
            rc_(src_of(o), src_of(o), ssem.at[o], ssem.at[o], o, j).wait_send()

        loop(E - 1, body)

    class Tree:
        def __init__(self, buf, own, recv, sz, s2, s3, hook):
            self.buf, self.own, self.recv = buf, own, recv
            self.sz, self.s2, self.s3, self.hook = sz, s2, s3, hook

        def send(self, blk, ssem, chip, src=None):
            src = self.buf.at[blk] if src is None else src
            rc_(src, self.buf.at[blk], ssem, self.recv.at[blk], chip, j).start()

        def wait(self, blk):
            rc_(self.buf.at[blk], self.buf.at[blk], self.recv.at[blk], self.recv.at[blk], p2, j).wait_recv()

        def start(self):
            self.send(me, self.s3.at[0], p3, self.own)
            self.send(me, self.s2.at[0], p2, self.own)

            def body(i):
                self.send(me, self.sz.at[i], ((a + i + 1) % A) * 4 + r, self.own)

            loop(A - 1, body)
            self.hook(me, self.own)

        def stage_z(self):
            def body(i):
                blk = ((a + i + 1) % A) * 4 + r
                self.wait(blk)
                self.send(blk, self.s3.at[i + 1], p3)
                self.send(blk, self.s2.at[i + 1], p2)
                self.hook(blk, self.buf.at[blk])

            loop(A - 1, body)

        def stage_2(self):
            def body(i):
                blk = ((a + i) % A) * 4 + r2
                self.wait(blk)
                self.send(blk, self.s3.at[A + i], p3)
                self.hook(blk, self.buf.at[blk])

            loop(A, body)

        def stage_3(self):
            for rr in (r3, r23):
                def body(i):
                    blk = ((a + i) % A) * 4 + rr
                    self.wait(blk)
                    self.hook(blk, self.buf.at[blk])

                loop(A, body)

        def drain(self):
            def one(sem):
                rc_(self.own, self.own, sem, sem, p2, j).wait_send()

            loop(A - 1, lambda i: one(self.sz.at[i]))
            loop(A, lambda i: one(self.s2.at[i]))
            loop(2 * A, lambda i: one(self.s3.at[i]))

    class Reduce:
        def __init__(self, part, b3, b2, bz, s3, v3, s2, v2, sz, vz):
            self.part, self.b3, self.b2, self.bz = part, b3, b2, bz
            self.s3, self.v3, self.s2, self.v2, self.sz, self.vz = s3, v3, s2, v2, sz, vz

        def copy3(self, i):
            first = 1 - i // A
            blk = (i % A) * 4 + r23 * first + r3 * (1 - first)
            return rc_(self.part.at[blk], self.b3.at[i], self.s3.at[i], self.v3.at[i], p3, j)

        def copy2(self, i):
            return rc_(self.part.at[i * 4 + r2], self.b2.at[i], self.s2.at[i], self.v2.at[i], p2, j)

        def copyz(self, o):
            return rc_(
                self.part.at[o * 4 + r], self.bz.at[a], self.sz.at[o], self.vz.at[a], o * 4 + r, j
            )

        def start(self):
            loop(2 * A, lambda i: self.copy3(i).start())

        def stage_2(self):
            def body(i):
                self.copy3(i).wait_recv()
                blk = i * 4 + r2
                self.part[blk] = (
                    self.part[blk].astype(jnp.float32) + self.b3[i].astype(jnp.float32)
                ).astype(jnp.bfloat16)
                self.copy2(i).start()

            loop(A, body)

        def stage_z(self):
            def total(o):
                self.copy3(A + o).wait_recv()
                self.copy2(o).wait_recv()
                return (
                    self.part[o * 4 + r].astype(jnp.float32)
                    + self.b3[A + o].astype(jnp.float32)
                    + self.b2[o].astype(jnp.float32)
                ).astype(jnp.bfloat16)

            def body(i):
                o = (a + i + 1) % A
                self.part[o * 4 + r] = total(o)
                self.copyz(o).start()

            loop(A - 1, body)
            self.bz[a] = total(a)

        def finish(self):
            def body(i):
                o = (a + i + 1) % A
                rc_(self.bz.at[o], self.bz.at[o], self.sz.at[o], self.vz.at[o], p2, j).wait_recv()

            loop(A - 1, body)
            out = self.bz[0].astype(jnp.float32)
            for i in range(1, A):
                out = out + self.bz[i].astype(jnp.float32)
            return out

        def drain(self):
            loop(2 * A, lambda i: self.copy3(i).wait_send())
            loop(A, lambda i: self.copy2(i).wait_send())
            loop(A - 1, lambda i: self.copyz((a + i + 1) % A).wait_send())

    def pair_hook(blk, src):
        if F > 1:
            for d in range(1, T):
                rc_(
                    src, gbuf.at[j, blk], g_ps.at[d, blk], g_pr.at[j, blk], me, (j + d) % T
                ).start()

    tree_g = Tree(gbuf.at[fj], own_g, g_recv, g_sz, g_s2, g_s3, pair_hook)
    tree_s = Tree(s3buf, s3buf.at[me], s3_recv, s3_sz, s3_s2, s3_s3, lambda blk, src: None)

    red_q = Reduce(ps, q3buf, q2buf, qzbuf, q3_s, q3_r, q2_s, q2_r, qz_s, qz_r)
    red_r = []
    for c in range(NC):
        cols = pl.ds(0, LANES + HC) if c == 0 else pl.ds(LANES, HC)
        red_r.append(
            Reduce(
                part.at[c, :, :, cols], r3buf.at[c, :, :, cols], r2buf.at[c, :, :, cols],
                rzbuf.at[c, :, :, cols], r3_s.at[c], r3_r.at[c], r2_s.at[c], r2_r.at[c],
                rz_s.at[c], rz_r.at[c],
            )
        )

    tree_g.start()

    fgroup = E // F
    offset = LANES + (me % fgroup) * DS
    WIN = sdpad.shape[0]
    low = jnp.minimum(offset // LANES, (LANES + H - WIN) // LANES) * LANES
    wcopies[0].wait()
    sdpad[pl.ds(pl.multiple_of(offset - low, 8), DS), :] = sd[...].astype(jnp.float32)

    tree_g.stage_z()
    tree_g.stage_2()
    tree_g.stage_3()
    for d in range(1, F):
        other = (j + d) % T

        def arrived(i):
            ref = gbuf.at[other, i]
            rc_(ref, ref, g_pr.at[other, i], g_pr.at[other, i], me, other).wait_recv()

        loop(E, arrived)

    window = flat(gbuf[me // fgroup, :, :, pl.ds(pl.multiple_of(low, LANES), WIN)])
    partial = jnp.dot(
        window, sdpad[...].astype(jnp.bfloat16), preferred_element_type=jnp.float32
    )
    ps[...] = partial.astype(jnp.bfloat16).reshape(E, tok, FFl)
    red_q.start()

    meta = flat(gbuf[fj, :, :, 0:LANES]).astype(jnp.float32)
    lane = lax.broadcasted_iota(jnp.int32, (tokens, LANES), 1)
    hit = jnp.where((meta == me.astype(jnp.float32)) & (lane < TOP), 1.0, 0.0)
    gates = pltpu.roll(meta, LANES - TOP, 1) + pltpu.roll(meta, LANES - 2 * TOP, 1)
    chosen = jnp.sum(hit, axis=1, keepdims=True)
    gate = jnp.sum(hit * gates, axis=1, keepdims=True)
    wide = jnp.broadcast_to(chosen, (tokens, LANES))
    row = lax.broadcasted_iota(jnp.int32, (tokens, LANES), 0) % tok
    total = wide
    shift = 1
    while shift < tok:
        total = total + jnp.where(row >= shift, pltpu.roll(total, shift, 0), 0.0)
        shift *= 2
    position = (total - wide)[:, :1]
    slots = sr.shape[1]
    cap = slots // E
    base = (lax.broadcasted_iota(jnp.int32, (tokens, 1), 0) // tok) * cap
    target = position + base.astype(jnp.float32)
    slot = lax.broadcasted_iota(jnp.int32, (tokens, slots), 1).astype(jnp.float32)
    permute = jnp.where((slot == target) & (chosen > 0.5), 1.0, 0.0).astype(jnp.bfloat16)
    wcopies[1].wait()
    pre_gate = jnp.dot(permute, sr[0], preferred_element_type=jnp.float32)
    pre_up = jnp.dot(permute, sr[1], preferred_element_type=jnp.float32)
    sig = jax.nn.sigmoid(pre_gate)
    d_up = pre_gate * sig
    d_gate = pre_up * sig * (1.0 + pre_gate * (1.0 - sig))

    wcopies[2].wait()

    def back_of(t):
        return dot_nt(flat(gbuf[t, :, :, LANES:]), wd[:, pl.ds(pl.multiple_of(t * H, LANES), H)])

    if F > 1:
        back = back_of(j)
        for d in range(1, T):
            other = (j + d) % T

            back = back + back_of(other)
    else:
        back = dot_nt(flat(gbuf[0, :, :, LANES:]), wd[...])
    red_q.stage_2()
    grad_up = back * d_up
    gate_sum = jnp.sum(grad_up * pre_up, axis=1, keepdims=True)
    grad_gate = (back * d_gate * gate).astype(jnp.bfloat16)
    grad_up = (grad_up * gate).astype(jnp.bfloat16)
    place = j * E + me if T * E <= LANES else me
    gate_row = jnp.where(lane == place, gate_sum, 0.0).astype(jnp.bfloat16)

    wcopies[4].wait()

    def rows_of(t, c):
        span = pl.ds(pl.multiple_of(t * HR + c * HC, 16), HC)
        return dot_nt(grad_gate, wgu[0, span, :]) + dot_nt(grad_up, wgu[1, span, :])

    for c in range(NC):
        for d in range(1, T):
            t = (j + d) % T
            pairsend[d - 1, c, :, LANES:] = rows_of(t, c).astype(jnp.bfloat16)
            if c == 0:
                pairsend[d - 1, c, :, 0:LANES] = gate_row
            rc_(
                pairsend.at[d - 1, c], pairbuf.at[T - 1 - d, c],
                pair_s.at[d - 1, c], pair_r.at[T - 1 - d, c], me, t,
            ).start()

    red_q.stage_z()

    def hidden_of_shared():
        shared_back = red_q.finish()
        sh = sv_ref[0].astype(jnp.float32)
        su = sv_ref[1].astype(jnp.float32)
        ssig = jax.nn.sigmoid(sh)
        s3buf[me, 0] = (shared_back * su * ssig * (1.0 + sh * (1.0 - ssig))).astype(jnp.bfloat16)
        s3buf[me, 1] = (shared_back * sh * ssig).astype(jnp.bfloat16)
        tree_s.start()

    for c in range(NC):
        mine = rows_of(j, c)
        for d in range(1, T):
            rc_(
                pairsend.at[d - 1, c], pairbuf.at[d - 1, c],
                pair_s.at[d - 1, c], pair_r.at[d - 1, c], me, (j + d) % T,
            ).wait_recv()
            mine = mine + pairbuf[d - 1, c, :, LANES:].astype(jnp.float32)
        part[c, :, :, LANES:] = mine.astype(jnp.bfloat16).reshape(E, tok, HC)
        if c == 0:
            sums = gate_row.astype(jnp.float32)
            for d in range(1, T):
                sums = sums + pairbuf[d - 1, c, :, 0:LANES].astype(jnp.float32)
            part[c, :, :, 0:LANES] = sums.astype(jnp.bfloat16).reshape(E, tok, LANES)
        red_r[c].start()
        if c == 0:
            hidden_of_shared()

    red_r[0].stage_2()
    tree_s.stage_z()
    red_r[0].stage_z()
    tree_s.stage_2()
    if NC > 1:
        red_r[1].stage_2()

    tree_s.stage_3()
    wcopies[3].wait()
    term = dot_nt(flat(s3buf[:, 0]), sgu[0]) + dot_nt(flat(s3buf[:, 1]), sgu[1])
    st[...] = term.astype(jnp.bfloat16).reshape(E, tok, st.shape[2])
    a2a_send(lambda o: st.at[o], s4buf, s4_s, s4_r)
    s4buf[me] = st[me]

    tree_g.drain()
    red_q.drain()
    if F > 1:
        for d in range(1, T):
            loop(
                E,
                lambda i: rc_(
                    gbuf.at[j, i], gbuf.at[j, i], g_ps.at[d, i], g_ps.at[d, i], me, (j + d) % T
                ).wait_send(),
            )

    if NC > 1:
        red_r[1].stage_z()
    tree_s.drain()

    a2a_wait(s4buf, s4_r)
    group = E // T
    for d in range(1, T):
        t = (j + d) % T
        rc_(
            s4buf.at[pl.ds(t * group, group)], s4pair.at[T - 1 - d],
            s4p_s.at[d - 1], s4p_r.at[T - 1 - d], me, t,
        ).start()
    shared = s4buf[pl.ds(j * group, group)].astype(jnp.float32)
    for d in range(1, T):
        rc_(
            s4pair.at[d - 1], s4pair.at[d - 1], s4p_s.at[d - 1], s4p_r.at[d - 1], me, (j + d) % T
        ).wait_recv()
        shared = shared + s4pair[d - 1].astype(jnp.float32)
    for o in range(group):
        spread[:, o * DS:(o + 1) * DS] = shared[o]
    a2a_drain(lambda o: st.at[o], s4_s)
    for d in range(1, T):
        rc_(
            s4pair.at[d - 1], s4pair.at[d - 1], s4p_s.at[d - 1], s4p_s.at[d - 1], me, (j + d) % T
        ).wait_send()
        for c in range(NC):
            ref = pairsend.at[d - 1, c]
            rc_(ref, ref, pair_s.at[d - 1, c], pair_s.at[d - 1, c], me, (j + d) % T).wait_send()

    done = [red_r[c].finish() for c in range(NC)]
    for c in range(NC):
        rows = done[c][:, LANES:] if c == 0 else done[c]
        out_r[:, c * HC:(c + 1) * HC] = rows + spread[:, c * HC:(c + 1) * HC]
    sums = done[0][:, 0:LANES]
    lane16 = lax.broadcasted_iota(jnp.int32, (tok, LANES), 1)
    expert_f = (lane16 % E).astype(jnp.float32)
    for parity in range(2):
        some = jnp.where(lane16 % 2 == parity, sums, 0.0)
        result = jnp.zeros((tok, LANES), jnp.float32)
        for k in range(TOP):
            value = jnp.sum(
                jnp.where(expert_f == own_meta[:, k:k + 1], some, 0.0), axis=1, keepdims=True
            )
            result = jnp.where(lane16 == k, value, result)
        square[0:tok] = result
        out_g[parity] = square[...].T[0:TOP, 0:tok]
    for c in range(NC):
        red_r[c].drain()


def per_device(
    E, T,
    grad_out, expert_ids, gate_values, w_gate_up, w_down, saved_routed,
    shared_gate_up, shared_down, saved_shared,
):
    tok, D = grad_out.shape
    TOP = expert_ids.shape[1]
    FFl = w_down.shape[1]
    DS = shared_down.shape[1]
    slots = saved_routed.shape[2]
    F = T if (D // T) % LANES == 0 else 1
    H = D // F
    HR = D // T
    NC = 2 if HR % (2 * LANES) == 0 else 1
    HC = HR // NC
    A = E // 4
    tokens = E * tok
    bf, f32 = jnp.bfloat16, jnp.float32
    V, S = pltpu.VMEM, pltpu.SemaphoreType.DMA
    T1 = max(T - 1, 1)
    W = LANES + HC
    WIN = (DS + LANES + LANES - 1) // LANES * LANES
    scratch = [
        V((LANES, LANES), f32), V((tok, HR), f32),
        V((F, E, tok, LANES + H), bf), V((DS, FFl), bf), V((WIN, FFl), f32),
        V((2, slots, FFl), bf), V((FFl, D), bf), V((2, DS, FFl), bf), V((2, D, FFl), bf),
        V((E, tok, FFl), bf), V((2 * A, tok, FFl), bf), V((A, tok, FFl), bf), V((A, tok, FFl), bf),
        V((E, 2, tok, FFl), bf),
        V((E, tok, DS), bf), V((E, tok, DS), bf), V((T1, E // T, tok, DS), bf),
        V((T1, NC, tokens, W), bf), V((T1, NC, tokens, W), bf), V((NC, E, tok, W), bf),
        V((NC, 2 * A, tok, W), bf), V((NC, A, tok, W), bf), V((NC, A, tok, W), bf),
        S((5,)), S((E,)), S((A,)), S((A,)), S((2 * A,)), S((T, E)), S((T, E)),
        S((E,)), S((A,)), S((A,)), S((2 * A,)),
        S((E,)), S((E,)), S((T1,)), S((T1,)), S((T1, NC)), S((T1, NC)),
        S((NC, 2 * A)), S((NC, 2 * A)), S((NC, A)), S((NC, A)), S((NC, A)), S((NC, A)),
        S((2 * A,)), S((2 * A,)), S((A,)), S((A,)), S((A,)), S((A,)),
    ]
    vm = pl.BlockSpec(memory_space=pltpu.VMEM)
    hbm = pl.BlockSpec(memory_space=pltpu.HBM)
    grad_in, gates = pl.pallas_call(
        functools.partial(kernel, E, T, F, NC, TOP),
        out_shape=(
            jax.ShapeDtypeStruct((tok, HR), f32),
            jax.ShapeDtypeStruct((2, TOP, tok), f32),
        ),
        in_specs=[vm] * 4 + [hbm] * 5,
        out_specs=(vm, vm),
        scratch_shapes=scratch,
        compiler_params=pltpu.CompilerParams(
            collective_id=0, has_side_effects=True, vmem_limit_bytes=60 * 1024 * 1024
        ),
    )(
        grad_out, expert_ids.T, gate_values.T, saved_shared, shared_down.T, saved_routed[0],
        w_down[0], shared_gate_up, w_gate_up[0],
    )
    return grad_in.astype(bf), (gates[0] + gates[1]).T


def solution(mesh):
    return jax.shard_map(
        functools.partial(per_device, mesh.shape["expert"], mesh.shape["tensor"]),
        mesh=mesh,
        in_specs=(
            P("expert", None),
            P("expert", None),
            P("expert", None),
            P("expert", None, None, "tensor"),
            P("expert", "tensor", None),
            P("expert", None, None, "tensor"),
            P(None, "expert", "tensor"),
            P("tensor", "expert"),
            P(None, "expert", "tensor"),
        ),
        out_specs=(P("expert", "tensor"), P("expert", None)),
        check_vma=False,
    )
```

```python
import functools

import jax
import jax.numpy as jnp
from jax import lax
from jax.experimental import pallas as pl
from jax.experimental.pallas import tpu as pltpu
from jax.sharding import PartitionSpec as P

MESH = pl.DeviceIdType.MESH
LANES = 128


def dot_nt(left, right):
    return lax.dot_general(
        left, right, (((1,), (1,)), ((), ())), preferred_element_type=jnp.float32
    )


def loop(count, body):
    def step(i, carry):
        body(i)
        return carry

    lax.fori_loop(0, count, step, 0)


def flat(value):
    return value.reshape(-1, value.shape[-1])


def kernel(
    E, T, F, NC, TOP,
    g_ref, id_ref, gv_ref, sv_ref, sd_hbm, sr_hbm, wd_hbm, sgu_hbm, wgu_hbm,
    out_r, out_g,
    square, spread, gbuf, sd, sdpad, sr, wd, sgu, wgu,
    ps, q3buf, q2buf, qzbuf, s3buf, st, s4buf, s4pair,
    pairsend, pairbuf, part, r3buf, r2buf, rzbuf,
    wsem, g_recv, g_sz, g_s2, g_s3, g_ps, g_pr,
    s3_recv, s3_sz, s3_s2, s3_s3,
    s4_s, s4_r, s4p_s, s4p_r, pair_s, pair_r,
    r3_s, r3_r, r2_s, r2_r, rz_s, rz_r,
    q3_s, q3_r, q2_s, q2_r, qz_s, qz_r,
):
    me = lax.axis_index("expert")
    j = lax.axis_index("tensor")
    A = E // 4
    a = me // 4
    r = me % 4
    rc = r + 1 - 2 * (r % 2)
    rb = r + 2 - 4 * (r // 2)
    odd = j % 2
    r2 = rc * (1 - odd) + rb * odd
    r3 = rb * (1 - odd) + rc * odd
    r23 = 3 - r
    p2 = a * 4 + r2
    p3 = a * 4 + r3
    fj = j if F > 1 else 0
    tok = g_ref.shape[0]
    DS = sd.shape[0]
    FFl = wd.shape[0]
    H = gbuf.shape[3] - LANES
    own_g = gbuf.at[fj, me]
    HC = part.shape[3] - LANES
    HR = HC * NC
    tokens = E * tok

    def rc_(src, dst, ssem, rsem, chip, core):
        return pltpu.make_async_remote_copy(
            src_ref=src, dst_ref=dst, send_sem=ssem, recv_sem=rsem,
            device_id=(chip, core), device_id_type=MESH,
        )

    wcopies = [
        pltpu.make_async_copy(sd_hbm, sd, wsem.at[0]),
        pltpu.make_async_copy(sr_hbm, sr, wsem.at[1]),
        pltpu.make_async_copy(wd_hbm, wd, wsem.at[2]),
        pltpu.make_async_copy(sgu_hbm, sgu, wsem.at[3]),
        pltpu.make_async_copy(wgu_hbm, wgu, wsem.at[4]),
    ]
    for copy in wcopies:
        copy.start()

    barrier = pltpu.get_barrier_semaphore()

    def greet(i):
        pl.semaphore_signal(barrier, inc=1, device_id=((me + i + 1) % E, j), device_id_type=MESH)

    loop(E - 1, greet)
    for d in range(1, T):
        pl.semaphore_signal(barrier, inc=1, device_id=(me, (j + d) % T), device_id_type=MESH)

    sdpad[...] = jnp.zeros_like(sdpad)
    square[...] = jnp.zeros_like(square)
    square[0:TOP, 0:tok] = id_ref[...].astype(jnp.float32)
    high = gv_ref[...].astype(jnp.bfloat16).astype(jnp.float32)
    square[TOP:2 * TOP, 0:tok] = high
    square[2 * TOP:3 * TOP, 0:tok] = gv_ref[...] - high
    own_meta = square[...].T[0:tok]
    gbuf[fj, me, :, 0:LANES] = own_meta.astype(jnp.bfloat16)
    if F > 1:
        gbuf[fj, me, :, LANES:] = g_ref[:, pl.ds(pl.multiple_of(fj * H, LANES), H)]
    else:
        gbuf[fj, me, :, LANES:] = g_ref[...]

    pl.semaphore_wait(barrier, E - 1 + T - 1)

    def a2a_send(src_of, dst, ssem, rsem):
        def body(i):
            o = (me + i + 1) % E
            rc_(src_of(o), dst.at[me], ssem.at[o], rsem.at[me], o, j).start()

        loop(E - 1, body)

    def a2a_wait(dst, rsem):
        def body(i):
            o = (me + i + 1) % E
            rc_(dst.at[o], dst.at[o], rsem.at[o], rsem.at[o], o, j).wait_recv()

        loop(E - 1, body)

    def a2a_drain(src_of, ssem):
        def body(i):
            o = (me + i + 1) % E
            rc_(src_of(o), src_of(o), ssem.at[o], ssem.at[o], o, j).wait_send()

        loop(E - 1, body)

    class Tree:
        def __init__(self, buf, own, recv, sz, s2, s3, hook):
            self.buf, self.own, self.recv = buf, own, recv
            self.sz, self.s2, self.s3, self.hook = sz, s2, s3, hook

        def send(self, blk, ssem, chip, src=None):
            src = self.buf.at[blk] if src is None else src
            rc_(src, self.buf.at[blk], ssem, self.recv.at[blk], chip, j).start()

        def wait(self, blk):
            rc_(self.buf.at[blk], self.buf.at[blk], self.recv.at[blk], self.recv.at[blk], p2, j).wait_recv()

        def start(self):
            self.send(me, self.s3.at[0], p3, self.own)
            self.send(me, self.s2.at[0], p2, self.own)

            def body(i):
                self.send(me, self.sz.at[i], ((a + i + 1) % A) * 4 + r, self.own)

            loop(A - 1, body)
            self.hook(me, self.own)

        def stage_z(self):
            def body(i):
                blk = ((a + i + 1) % A) * 4 + r
                self.wait(blk)
                self.send(blk, self.s3.at[i + 1], p3)
                self.send(blk, self.s2.at[i + 1], p2)
                self.hook(blk, self.buf.at[blk])

            loop(A - 1, body)

        def stage_2(self):
            def body(i):
                blk = ((a + i) % A) * 4 + r2
                self.wait(blk)
                self.send(blk, self.s3.at[A + i], p3)
                self.hook(blk, self.buf.at[blk])

            loop(A, body)

        def stage_3(self):
            for rr in (r3, r23):
                def body(i):
                    blk = ((a + i) % A) * 4 + rr
                    self.wait(blk)
                    self.hook(blk, self.buf.at[blk])

                loop(A, body)

        def drain(self):
            def one(sem):
                rc_(self.own, self.own, sem, sem, p2, j).wait_send()

            loop(A - 1, lambda i: one(self.sz.at[i]))
            loop(A, lambda i: one(self.s2.at[i]))
            loop(2 * A, lambda i: one(self.s3.at[i]))

    class Reduce:
        def __init__(self, part, b3, b2, bz, s3, v3, s2, v2, sz, vz):
            self.part, self.b3, self.b2, self.bz = part, b3, b2, bz
            self.s3, self.v3, self.s2, self.v2, self.sz, self.vz = s3, v3, s2, v2, sz, vz

        def copy3(self, i):
            first = 1 - i // A
            blk = (i % A) * 4 + r23 * first + r3 * (1 - first)
            return rc_(self.part.at[blk], self.b3.at[i], self.s3.at[i], self.v3.at[i], p3, j)

        def copy2(self, i):
            return rc_(self.part.at[i * 4 + r2], self.b2.at[i], self.s2.at[i], self.v2.at[i], p2, j)

        def copyz(self, o):
            return rc_(
                self.part.at[o * 4 + r], self.bz.at[a], self.sz.at[o], self.vz.at[a], o * 4 + r, j
            )

        def start(self):
            loop(2 * A, lambda i: self.copy3(i).start())

        def stage_2(self):
            def body(i):
                self.copy3(i).wait_recv()
                blk = i * 4 + r2
                self.part[blk] = (
                    self.part[blk].astype(jnp.float32) + self.b3[i].astype(jnp.float32)
                ).astype(jnp.bfloat16)
                self.copy2(i).start()

            loop(A, body)

        def stage_z(self):
            def total(o):
                self.copy3(A + o).wait_recv()
                self.copy2(o).wait_recv()
                return (
                    self.part[o * 4 + r].astype(jnp.float32)
                    + self.b3[A + o].astype(jnp.float32)
                    + self.b2[o].astype(jnp.float32)
                ).astype(jnp.bfloat16)

            def body(i):
                o = (a + i + 1) % A
                self.part[o * 4 + r] = total(o)
                self.copyz(o).start()

            loop(A - 1, body)
            self.bz[a] = total(a)

        def finish(self):
            def body(i):
                o = (a + i + 1) % A
                rc_(self.bz.at[o], self.bz.at[o], self.sz.at[o], self.vz.at[o], p2, j).wait_recv()

            loop(A - 1, body)
            out = self.bz[0].astype(jnp.float32)
            for i in range(1, A):
                out = out + self.bz[i].astype(jnp.float32)
            return out

        def drain(self):
            loop(2 * A, lambda i: self.copy3(i).wait_send())
            loop(A, lambda i: self.copy2(i).wait_send())
            loop(A - 1, lambda i: self.copyz((a + i + 1) % A).wait_send())

    def pair_hook(blk, src):
        if F > 1:
            for d in range(1, T):
                rc_(
                    src, gbuf.at[j, blk], g_ps.at[d, blk], g_pr.at[j, blk], me, (j + d) % T
                ).start()

    tree_g = Tree(gbuf.at[fj], own_g, g_recv, g_sz, g_s2, g_s3, pair_hook)
    tree_s = Tree(s3buf, s3buf.at[me], s3_recv, s3_sz, s3_s2, s3_s3, lambda blk, src: None)

    red_q = Reduce(ps, q3buf, q2buf, qzbuf, q3_s, q3_r, q2_s, q2_r, qz_s, qz_r)
    red_r = []
    for c in range(NC):
        cols = pl.ds(0, LANES + HC) if c == 0 else pl.ds(LANES, HC)
        red_r.append(
            Reduce(
                part.at[c, :, :, cols], r3buf.at[c, :, :, cols], r2buf.at[c, :, :, cols],
                rzbuf.at[c, :, :, cols], r3_s.at[c], r3_r.at[c], r2_s.at[c], r2_r.at[c],
                rz_s.at[c], rz_r.at[c],
            )
        )

    tree_g.start()

    fgroup = E // F
    offset = LANES + (me % fgroup) * DS
    WIN = sdpad.shape[0]
    low = jnp.minimum(offset // LANES, (LANES + H - WIN) // LANES) * LANES
    wcopies[0].wait()
    sdpad[pl.ds(pl.multiple_of(offset - low, 8), DS), :] = sd[...].astype(jnp.float32)

    tree_g.stage_z()
    tree_g.stage_2()
    tree_g.stage_3()
    for d in range(1, F):
        other = (j + d) % T

        def arrived(i):
            ref = gbuf.at[other, i]
            rc_(ref, ref, g_pr.at[other, i], g_pr.at[other, i], me, other).wait_recv()

        loop(E, arrived)

    window = flat(gbuf[me // fgroup, :, :, pl.ds(pl.multiple_of(low, LANES), WIN)])
    partial = jnp.dot(
        window, sdpad[...].astype(jnp.bfloat16), preferred_element_type=jnp.float32
    )
    ps[...] = partial.astype(jnp.bfloat16).reshape(E, tok, FFl)
    red_q.start()

    meta = flat(gbuf[fj, :, :, 0:LANES]).astype(jnp.float32)
    lane = lax.broadcasted_iota(jnp.int32, (tokens, LANES), 1)
    hit = jnp.where((meta == me.astype(jnp.float32)) & (lane < TOP), 1.0, 0.0)
    gates = pltpu.roll(meta, LANES - TOP, 1) + pltpu.roll(meta, LANES - 2 * TOP, 1)
    chosen = jnp.sum(hit, axis=1, keepdims=True)
    gate = jnp.sum(hit * gates, axis=1, keepdims=True)
    wide = jnp.broadcast_to(chosen, (tokens, LANES))
    row = lax.broadcasted_iota(jnp.int32, (tokens, LANES), 0) % tok
    total = wide
    shift = 1
    while shift < tok:
        total = total + jnp.where(row >= shift, pltpu.roll(total, shift, 0), 0.0)
        shift *= 2
    position = (total - wide)[:, :1]
    slots = sr.shape[1]
    cap = slots // E
    base = (lax.broadcasted_iota(jnp.int32, (tokens, 1), 0) // tok) * cap
    target = position + base.astype(jnp.float32)
    slot = lax.broadcasted_iota(jnp.int32, (tokens, slots), 1).astype(jnp.float32)
    permute = jnp.where((slot == target) & (chosen > 0.5), 1.0, 0.0).astype(jnp.bfloat16)
    wcopies[1].wait()
    pre_gate = jnp.dot(permute, sr[0], preferred_element_type=jnp.float32)
    pre_up = jnp.dot(permute, sr[1], preferred_element_type=jnp.float32)
    sig = jax.nn.sigmoid(pre_gate)
    d_up = pre_gate * sig
    d_gate = pre_up * sig * (1.0 + pre_gate * (1.0 - sig))

    wcopies[2].wait()

    def back_of(t):
        return dot_nt(flat(gbuf[t, :, :, LANES:]), wd[:, pl.ds(pl.multiple_of(t * H, LANES), H)])

    if F > 1:
        back = back_of(j)
        for d in range(1, T):
            other = (j + d) % T

            back = back + back_of(other)
    else:
        back = dot_nt(flat(gbuf[0, :, :, LANES:]), wd[...])
    red_q.stage_2()
    grad_up = back * d_up
    gate_sum = jnp.sum(grad_up * pre_up, axis=1, keepdims=True)
    grad_gate = (back * d_gate * gate).astype(jnp.bfloat16)
    grad_up = (grad_up * gate).astype(jnp.bfloat16)
    place = j * E + me if T * E <= LANES else me
    gate_row = jnp.where(lane == place, gate_sum, 0.0).astype(jnp.bfloat16)

    wcopies[4].wait()

    def rows_of(t, c):
        span = pl.ds(pl.multiple_of(t * HR + c * HC, 16), HC)
        return dot_nt(grad_gate, wgu[0, span, :]) + dot_nt(grad_up, wgu[1, span, :])

    for c in range(NC):
        for d in range(1, T):
            t = (j + d) % T
            pairsend[d - 1, c, :, LANES:] = rows_of(t, c).astype(jnp.bfloat16)
            if c == 0:
                pairsend[d - 1, c, :, 0:LANES] = gate_row
            rc_(
                pairsend.at[d - 1, c], pairbuf.at[T - 1 - d, c],
                pair_s.at[d - 1, c], pair_r.at[T - 1 - d, c], me, t,
            ).start()

    red_q.stage_z()

    def hidden_of_shared():
        shared_back = red_q.finish()
        sh = sv_ref[0].astype(jnp.float32)
        su = sv_ref[1].astype(jnp.float32)
        ssig = jax.nn.sigmoid(sh)
        s3buf[me, 0] = (shared_back * su * ssig * (1.0 + sh * (1.0 - ssig))).astype(jnp.bfloat16)
        s3buf[me, 1] = (shared_back * sh * ssig).astype(jnp.bfloat16)
        tree_s.start()

    hidden_of_shared()
    for c in range(NC):
        mine = rows_of(j, c)
        for d in range(1, T):
            rc_(
                pairsend.at[d - 1, c], pairbuf.at[d - 1, c],
                pair_s.at[d - 1, c], pair_r.at[d - 1, c], me, (j + d) % T,
            ).wait_recv()
            mine = mine + pairbuf[d - 1, c, :, LANES:].astype(jnp.float32)
        part[c, :, :, LANES:] = mine.astype(jnp.bfloat16).reshape(E, tok, HC)
        if c == 0:
            sums = gate_row.astype(jnp.float32)
            for d in range(1, T):
                sums = sums + pairbuf[d - 1, c, :, 0:LANES].astype(jnp.float32)
            part[c, :, :, 0:LANES] = sums.astype(jnp.bfloat16).reshape(E, tok, LANES)
        red_r[c].start()
        if c == 0:
            tree_s.stage_z()

    tree_s.stage_2()
    red_r[0].stage_2()

    tree_s.stage_3()
    wcopies[3].wait()
    term = dot_nt(flat(s3buf[:, 0]), sgu[0]) + dot_nt(flat(s3buf[:, 1]), sgu[1])
    st[...] = term.astype(jnp.bfloat16).reshape(E, tok, st.shape[2])
    a2a_send(lambda o: st.at[o], s4buf, s4_s, s4_r)
    s4buf[me] = st[me]

    red_r[0].stage_z()
    if NC > 1:
        red_r[1].stage_2()
    tree_g.drain()
    red_q.drain()
    if F > 1:
        for d in range(1, T):
            loop(
                E,
                lambda i: rc_(
                    gbuf.at[j, i], gbuf.at[j, i], g_ps.at[d, i], g_ps.at[d, i], me, (j + d) % T
                ).wait_send(),
            )

    if NC > 1:
        red_r[1].stage_z()
    tree_s.drain()

    a2a_wait(s4buf, s4_r)
    group = E // T
    for d in range(1, T):
        t = (j + d) % T
        rc_(
            s4buf.at[pl.ds(t * group, group)], s4pair.at[T - 1 - d],
            s4p_s.at[d - 1], s4p_r.at[T - 1 - d], me, t,
        ).start()
    shared = s4buf[pl.ds(j * group, group)].astype(jnp.float32)
    for d in range(1, T):
        rc_(
            s4pair.at[d - 1], s4pair.at[d - 1], s4p_s.at[d - 1], s4p_r.at[d - 1], me, (j + d) % T
        ).wait_recv()
        shared = shared + s4pair[d - 1].astype(jnp.float32)
    for o in range(group):
        spread[:, o * DS:(o + 1) * DS] = shared[o]
    a2a_drain(lambda o: st.at[o], s4_s)
    for d in range(1, T):
        rc_(
            s4pair.at[d - 1], s4pair.at[d - 1], s4p_s.at[d - 1], s4p_s.at[d - 1], me, (j + d) % T
        ).wait_send()
        for c in range(NC):
            ref = pairsend.at[d - 1, c]
            rc_(ref, ref, pair_s.at[d - 1, c], pair_s.at[d - 1, c], me, (j + d) % T).wait_send()

    done = [red_r[c].finish() for c in range(NC)]
    for c in range(NC):
        rows = done[c][:, LANES:] if c == 0 else done[c]
        out_r[:, c * HC:(c + 1) * HC] = rows + spread[:, c * HC:(c + 1) * HC]
    sums = done[0][:, 0:LANES]
    lane16 = lax.broadcasted_iota(jnp.int32, (tok, LANES), 1)
    expert_f = (lane16 % E).astype(jnp.float32)
    for parity in range(2):
        some = jnp.where(lane16 % 2 == parity, sums, 0.0)
        result = jnp.zeros((tok, LANES), jnp.float32)
        for k in range(TOP):
            value = jnp.sum(
                jnp.where(expert_f == own_meta[:, k:k + 1], some, 0.0), axis=1, keepdims=True
            )
            result = jnp.where(lane16 == k, value, result)
        square[0:tok] = result
        out_g[parity] = square[...].T[0:TOP, 0:tok]
    for c in range(NC):
        red_r[c].drain()


def per_device(
    E, T,
    grad_out, expert_ids, gate_values, w_gate_up, w_down, saved_routed,
    shared_gate_up, shared_down, saved_shared,
):
    tok, D = grad_out.shape
    TOP = expert_ids.shape[1]
    FFl = w_down.shape[1]
    DS = shared_down.shape[1]
    slots = saved_routed.shape[2]
    F = T if (D // T) % LANES == 0 else 1
    H = D // F
    HR = D // T
    NC = 2 if HR % (2 * LANES) == 0 else 1
    HC = HR // NC
    A = E // 4
    tokens = E * tok
    bf, f32 = jnp.bfloat16, jnp.float32
    V, S = pltpu.VMEM, pltpu.SemaphoreType.DMA
    T1 = max(T - 1, 1)
    W = LANES + HC
    WIN = (DS + LANES + LANES - 1) // LANES * LANES
    scratch = [
        V((LANES, LANES), f32), V((tok, HR), f32),
        V((F, E, tok, LANES + H), bf), V((DS, FFl), bf), V((WIN, FFl), f32),
        V((2, slots, FFl), bf), V((FFl, D), bf), V((2, DS, FFl), bf), V((2, D, FFl), bf),
        V((E, tok, FFl), bf), V((2 * A, tok, FFl), bf), V((A, tok, FFl), bf), V((A, tok, FFl), bf),
        V((E, 2, tok, FFl), bf),
        V((E, tok, DS), bf), V((E, tok, DS), bf), V((T1, E // T, tok, DS), bf),
        V((T1, NC, tokens, W), bf), V((T1, NC, tokens, W), bf), V((NC, E, tok, W), bf),
        V((NC, 2 * A, tok, W), bf), V((NC, A, tok, W), bf), V((NC, A, tok, W), bf),
        S((5,)), S((E,)), S((A,)), S((A,)), S((2 * A,)), S((T, E)), S((T, E)),
        S((E,)), S((A,)), S((A,)), S((2 * A,)),
        S((E,)), S((E,)), S((T1,)), S((T1,)), S((T1, NC)), S((T1, NC)),
        S((NC, 2 * A)), S((NC, 2 * A)), S((NC, A)), S((NC, A)), S((NC, A)), S((NC, A)),
        S((2 * A,)), S((2 * A,)), S((A,)), S((A,)), S((A,)), S((A,)),
    ]
    vm = pl.BlockSpec(memory_space=pltpu.VMEM)
    hbm = pl.BlockSpec(memory_space=pltpu.HBM)
    grad_in, gates = pl.pallas_call(
        functools.partial(kernel, E, T, F, NC, TOP),
        out_shape=(
            jax.ShapeDtypeStruct((tok, HR), f32),
            jax.ShapeDtypeStruct((2, TOP, tok), f32),
        ),
        in_specs=[vm] * 4 + [hbm] * 5,
        out_specs=(vm, vm),
        scratch_shapes=scratch,
        compiler_params=pltpu.CompilerParams(
            collective_id=0, has_side_effects=True, vmem_limit_bytes=60 * 1024 * 1024
        ),
    )(
        grad_out, expert_ids.T, gate_values.T, saved_shared, shared_down.T, saved_routed[0],
        w_down[0], shared_gate_up, w_gate_up[0],
    )
    return grad_in.astype(bf), (gates[0] + gates[1]).T


def solution(mesh):
    return jax.shard_map(
        functools.partial(per_device, mesh.shape["expert"], mesh.shape["tensor"]),
        mesh=mesh,
        in_specs=(
            P("expert", None),
            P("expert", None),
            P("expert", None),
            P("expert", None, None, "tensor"),
            P("expert", "tensor", None),
            P("expert", None, None, "tensor"),
            P(None, "expert", "tensor"),
            P("tensor", "expert"),
            P(None, "expert", "tensor"),
        ),
        out_specs=(P("expert", "tensor"), P("expert", None)),
        check_vma=False,
    )
```
